32 devices in a mesh: batch: 4 (over z), grid: 8 (over y, x, core).
Axes of the slice: x: 2, y: 2, z: 4, core: 2. Of those that a mesh axis runs over, the one named last changes fastest.
Arguments:
- fields: bfloat16 [1024, 512, 512], P(('batch', 'grid')), parts along dimension 0, may hold values from -18 to 18
- norm_gain: float32 [256], replicated, may hold values from 0.5 to 1.5
- norm_shift: float32 [256], replicated, may hold values from -3 to 3
- first_weight: bfloat16 [2, 8, 32, 32], replicated, may hold values from -0.75 to 0.75
- second_weight: bfloat16 [2, 8, 32, 32], replicated, may hold values from -0.75 to 0.75
- first_bias: float32 [2, 256], replicated, may hold values from -2 to 2
Outputs:
- mixed_fields: bfloat16 [1024, 512, 512], P(('batch', 'grid')), parts along dimension 0
The draws below stay inside these ranges and needn't reach their ends.
There are 4 independent parts, one for each index of `batch`. The reference program is written for one: setup_inputs(seed, part) draws one part's arguments, and reference() takes and returns one part's arrays. A program takes and returns all parts, laid end to end along the dimension named above; an argument that names none is the same for every part. Nothing has to cross between parts.
All inputs are finite; a program needn't handle non-finite values.
Results may differ from the reference program's by a relative error of at most 0.0055.
Values may be sent and summed in bfloat16 or wider, within the bound.
A program may use at most 192 MiB of HBM per device.

```python
import math
import jax
import jax.numpy as jnp
from jax import lax

C = 256
BS = 32
H = 512
W = 512
NB = 8


def draw_fields(key, part):
    first_key = jax.random.fold_in(key, 11)
    ramp = jnp.arange(C, dtype=jnp.float32) / (C - 1)
    base = jnp.clip(jax.random.normal(first_key, (C, H, W), jnp.float32), -4.0, 4.0)
    scale = jnp.power(3.0, ramp)
    return (base * scale[:, None, None]).astype(jnp.bfloat16)


def normal_values(key, extent, scale, bound, kind=jnp.bfloat16):
    entries = scale * jax.random.normal(key, extent, jnp.float32)
    return jnp.clip(entries, min=-bound, max=bound).astype(kind)


def setup_inputs(seed: int = 0, part: int = 0) -> dict:
    splits = jax.random.split(jax.random.key(seed), 7)
    part_splits = jax.random.split(jax.random.fold_in(splits[6], part), 7)
    return {
        "fields": draw_fields(jax.random.fold_in(jax.random.fold_in(splits[6], part), 71), part),
        "norm_gain": jnp.clip(1.0 + 0.1 * jax.random.normal(splits[1], (C,), jnp.float32), 0.5, 1.5),
        "norm_shift": normal_values(splits[2], (C,), 0.5, 3.0, jnp.float32),
        "first_weight": normal_values(splits[3], (2, NB, BS, BS), (2 * BS) ** -0.5, 0.75),
        "second_weight": normal_values(splits[4], (2, NB, BS, BS), (2 * BS) ** -0.5, 0.75),
        "first_bias": normal_values(splits[5], (2, C), 0.3, 2.0, jnp.float32),
    }


def tables(rows, cols):
    half = cols // 2
    col_index = jnp.arange(cols, dtype=jnp.int32)
    mode_index = jnp.arange(half, dtype=jnp.int32)
    angle_w = (col_index[:, None] * mode_index[None, :] % cols).astype(jnp.float32) * (2.0 * math.pi / cols)
    scale_w = 1.0 / math.sqrt(cols)
    fwd_w = jnp.concatenate([jnp.cos(angle_w) * scale_w, -jnp.sin(angle_w) * scale_w], axis=1).astype(jnp.bfloat16)
    weight_k = jnp.where(mode_index == 0, 1.0, 2.0).astype(jnp.float32)
    inv_w = jnp.concatenate([(jnp.cos(angle_w) * weight_k[None, :] * scale_w).T, (-jnp.sin(angle_w) * weight_k[None, :] * scale_w).T], axis=0).astype(jnp.bfloat16)
    row_index = jnp.arange(rows, dtype=jnp.int32)
    angle_h = (row_index[:, None] * row_index[None, :] % rows).astype(jnp.float32) * (2.0 * math.pi / rows)
    scale_h = 1.0 / math.sqrt(rows)
    cos_h = (jnp.cos(angle_h) * scale_h).astype(jnp.bfloat16)
    sin_h = (jnp.sin(angle_h) * scale_h).astype(jnp.bfloat16)
    return (fwd_w, inv_w, cos_h, sin_h)

def mult(form, left, right):
    return jnp.einsum(form, left.astype(jnp.float32), right.astype(jnp.float32), precision=lax.Precision.HIGHEST)

def shrink(values):
    return jnp.maximum(values - 0.01, 0.0) + jnp.minimum(values + 0.01, 0.0)

def mix_modes(real_part, imag_part, first_weight, second_weight, first_bias):
    blocks = first_weight.shape[1]
    width = first_weight.shape[2]
    shape = real_part.shape
    real_blk = real_part.reshape(blocks, width, -1)
    imag_blk = imag_part.reshape(blocks, width, -1)
    bias_blk = first_bias.reshape(2, blocks, width, 1)
    hid_re = jax.nn.relu(mult('bio,bim->bom', first_weight[0], real_blk) - mult('bio,bim->bom', first_weight[1], imag_blk) + bias_blk[0]).astype(jnp.bfloat16)
    hid_im = jax.nn.relu(mult('bio,bim->bom', first_weight[0], imag_blk) + mult('bio,bim->bom', first_weight[1], real_blk) + bias_blk[1]).astype(jnp.bfloat16)
    out_re = mult('bio,bim->bom', second_weight[0], hid_re) - mult('bio,bim->bom', second_weight[1], hid_im)
    out_im = mult('bio,bim->bom', second_weight[0], hid_im) + mult('bio,bim->bom', second_weight[1], hid_re)
    return (shrink(out_re).astype(jnp.bfloat16).reshape(shape), shrink(out_im).astype(jnp.bfloat16).reshape(shape))

def reference(fields, norm_gain, norm_shift, first_weight, second_weight, first_bias):
    channels, rows, cols = fields.shape
    half = cols // 2
    fwd_w, inv_w, cos_h, sin_h = tables(rows, cols)
    values = fields.astype(jnp.float32)
    mean = lax.optimization_barrier(jnp.mean(values, axis=0))
    mean_sq = lax.optimization_barrier(jnp.mean(values * values, axis=0))
    var = mean_sq - mean * mean
    normed = ((values - mean) * lax.rsqrt(var + 1e-05) * norm_gain[:, None, None] + norm_shift[:, None, None]).astype(jnp.bfloat16)
    along_w = mult('chw,wk->chk', normed, fwd_w).astype(jnp.bfloat16).reshape(channels, rows, 2, half)
    first_p = mult('kh,chpq->ckpq', cos_h, along_w)
    first_q = mult('kh,chpq->ckpq', sin_h, along_w)
    modes_re = (first_p[:, :, 0] + first_q[:, :, 1]).astype(jnp.bfloat16)
    modes_im = (first_p[:, :, 1] - first_q[:, :, 0]).astype(jnp.bfloat16)
    shr_re, shr_im = mix_modes(modes_re, modes_im, first_weight, second_weight, first_bias)
    shrunk = jnp.stack([shr_re, shr_im], axis=2)
    back_p = mult('kh,ckpq->chpq', cos_h, shrunk)
    back_q = mult('kh,ckpq->chpq', sin_h, shrunk)
    back_re = (back_p[:, :, 0] - back_q[:, :, 1]).astype(jnp.bfloat16)
    back_im = (back_p[:, :, 1] + back_q[:, :, 0]).astype(jnp.bfloat16)
    backed = jnp.concatenate([back_re, back_im], axis=2)
    filtered = mult('chk,kw->chw', backed, inv_w)
    return (values + filtered).astype(jnp.bfloat16)
```

```python
import functools
import math

import jax
import jax.numpy as jnp
import numpy as np
from jax import lax
from jax.experimental import pallas as pl
from jax.experimental.pallas import tpu as pltpu
from jax.sharding import PartitionSpec as P


def tables(rows, cols):
    half = cols // 2
    col_index = jnp.arange(cols, dtype=jnp.int32)
    mode_index = jnp.arange(half, dtype=jnp.int32)
    angle_w = (col_index[:, None] * mode_index[None, :] % cols).astype(jnp.float32) * (
        2.0 * math.pi / cols
    )
    scale_w = 1.0 / math.sqrt(cols)
    fwd_w = jnp.concatenate(
        [jnp.cos(angle_w) * scale_w, -jnp.sin(angle_w) * scale_w], axis=1
    ).astype(jnp.bfloat16)
    weight_k = jnp.where(mode_index == 0, 1.0, 2.0).astype(jnp.float32)
    inv_w = jnp.concatenate(
        [
            (jnp.cos(angle_w) * weight_k[None, :] * scale_w).T,
            (-jnp.sin(angle_w) * weight_k[None, :] * scale_w).T,
        ],
        axis=0,
    ).astype(jnp.bfloat16)
    row_index = jnp.arange(rows, dtype=jnp.int32)
    angle_h = (row_index[:, None] * row_index[None, :] % rows).astype(jnp.float32) * (
        2.0 * math.pi / rows
    )
    scale_h = 1.0 / math.sqrt(rows)
    cos_h = (jnp.cos(angle_h) * scale_h).astype(jnp.bfloat16)
    sin_h = (jnp.sin(angle_h) * scale_h).astype(jnp.bfloat16)
    return (fwd_w, inv_w, cos_h, sin_h)


def mult(form, left, right):
    return jnp.einsum(form, left, right, preferred_element_type=jnp.float32)


def shrink(values):
    return jnp.maximum(values - 0.01, 0.0) + jnp.minimum(values + 0.01, 0.0)


def mix_modes(real_part, imag_part, first_weight, second_weight, first_bias):
    blocks = first_weight.shape[1]
    width = first_weight.shape[2]
    shape = real_part.shape
    real_blk = real_part.reshape(blocks, width, -1)
    imag_blk = imag_part.reshape(blocks, width, -1)
    bias_blk = first_bias.reshape(2, blocks, width, 1)
    hid_re = jax.nn.relu(
        mult("bio,bim->bom", first_weight[0], real_blk)
        - mult("bio,bim->bom", first_weight[1], imag_blk)
        + bias_blk[0]
    ).astype(jnp.bfloat16)
    hid_im = jax.nn.relu(
        mult("bio,bim->bom", first_weight[0], imag_blk)
        + mult("bio,bim->bom", first_weight[1], real_blk)
        + bias_blk[1]
    ).astype(jnp.bfloat16)
    out_re = mult("bio,bim->bom", second_weight[0], hid_re) - mult(
        "bio,bim->bom", second_weight[1], hid_im
    )
    out_im = mult("bio,bim->bom", second_weight[0], hid_im) + mult(
        "bio,bim->bom", second_weight[1], hid_re
    )
    return (
        shrink(out_re).astype(jnp.bfloat16).reshape(shape),
        shrink(out_im).astype(jnp.bfloat16).reshape(shape),
    )


def per_device(fields, norm_gain, norm_shift, first_weight, second_weight, first_bias):
    local_ch, rows, cols = fields.shape
    half = cols // 2
    groups = lax.axis_size("grid")
    channels = local_ch * groups
    fwd_w, inv_w, cos_h, sin_h = tables(rows, cols)
    values = fields.astype(jnp.float32)
    start = lax.axis_index("grid") * local_ch
    gain_own = lax.dynamic_slice_in_dim(norm_gain, start, local_ch)
    shift_own = lax.dynamic_slice_in_dim(norm_shift, start, local_ch)
    total_sum, total_sq = lax.psum(
        (jnp.sum(values, axis=0), jnp.sum(values * values, axis=0)), "grid"
    )
    mean = total_sum / channels
    var = total_sq / channels - mean * mean
    normed = (
        (values - mean) * lax.rsqrt(var + 1e-05) * gain_own[:, None, None]
        + shift_own[:, None, None]
    ).astype(jnp.bfloat16)
    along_w = (
        mult("chw,wk->chk", normed, fwd_w).astype(jnp.bfloat16).reshape(local_ch, rows, 2, half)
    )
    first_p = mult("kh,chpq->ckpq", cos_h, along_w)
    first_q = mult("kh,chpq->ckpq", sin_h, along_w)
    modes = jnp.stack(
        [
            (first_p[:, :, 0] + first_q[:, :, 1]).astype(jnp.bfloat16),
            (first_p[:, :, 1] - first_q[:, :, 0]).astype(jnp.bfloat16),
        ],
        axis=2,
    )
    spread = lax.all_to_all(modes, "grid", split_axis=1, concat_axis=0, tiled=True)
    shr_re, shr_im = mix_modes(
        spread[:, :, 0], spread[:, :, 1], first_weight, second_weight, first_bias
    )
    gathered = lax.all_to_all(
        jnp.stack([shr_re, shr_im], axis=2), "grid", split_axis=0, concat_axis=1, tiled=True
    )
    back_p = mult("kh,ckpq->chpq", cos_h, gathered)
    back_q = mult("kh,ckpq->chpq", sin_h, gathered)
    back_re = (back_p[:, :, 0] - back_q[:, :, 1]).astype(jnp.bfloat16)
    back_im = (back_p[:, :, 1] + back_q[:, :, 0]).astype(jnp.bfloat16)
    backed = jnp.concatenate([back_re, back_im], axis=2)
    filtered = mult("chk,kw->chw", backed, inv_w)
    return (values + filtered).astype(jnp.bfloat16)

SUB = 8


def stats_kernel(n, channels, sum_ref, sq_ref, out_ref, near, part, far, s1, r1, s2, r2, s3, r3, s4, r4):
    me = lax.axis_index("grid")
    chips = n // 2
    core, chip = lax.rem(me, 2), lax.div(me, 2)
    other = 1 - core
    sibling = chip * 2 + other
    rows = sum_ref.shape[0]
    half, piece = rows // 2, rows // n

    def ahead(j):
        return lax.rem(chip + j, chips)

    def span(c, k):
        return pl.ds(pl.multiple_of(c * half + k * piece, 8), piece)

    def send(source, target, send_sem, recv_sem, device):
        copy = pltpu.make_async_remote_copy(
            src_ref=source,
            dst_ref=target,
            send_sem=send_sem,
            recv_sem=recv_sem,
            device_id={"grid": device},
            device_id_type=pl.DeviceIdType.MESH,
        )
        copy.start()
        return copy

    barrier = pltpu.get_barrier_semaphore()
    for device in [sibling] + [ahead(j) * 2 + core for j in range(1, chips)]:
        pl.semaphore_signal(
            barrier, inc=1, device_id={"grid": device}, device_id_type=pl.DeviceIdType.MESH
        )
    pl.semaphore_wait(barrier, chips)

    theirs = pl.ds(pl.multiple_of(other * half, 8), half)
    first = [
        send(ref.at[theirs], near.at[i], s1.at[i], r1.at[i], sibling)
        for i, ref in enumerate((sum_ref, sq_ref))
    ]
    for copy in first:
        copy.wait_recv()
    second = []
    for j in range(1, chips + 1):
        k = ahead(j)
        local = pl.ds(pl.multiple_of(k * piece, 8), piece)
        for i, ref in enumerate((sum_ref, sq_ref)):
            part[j - 1, i] = ref[span(core, k)] + near[i, local]
    for j in range(1, chips):
        second.append(
            send(part.at[j - 1], far.at[j - 1], s2.at[j - 1], r2.at[j - 1], ahead(j) * 2 + core)
        )
    total_sum, total_sq = part[chips - 1, 0], part[chips - 1, 1]
    for j in range(1, chips):
        second[j - 1].wait_recv()
        total_sum = total_sum + far[j - 1, 0]
        total_sq = total_sq + far[j - 1, 1]
    mean = total_sum * (1.0 / channels)
    mine = span(core, chip)
    out_ref[0, mine] = mean
    out_ref[1, mine] = lax.rsqrt(total_sq * (1.0 / channels) - mean * mean + 1e-05)
    block = out_ref.at[:, mine]
    third = [
        send(block, block, s3.at[j - 1], r3.at[j - 1], ahead(j) * 2 + core)
        for j in range(1, chips)
    ]
    fourth = [send(block, block, s4.at[0], r4.at[0], sibling)]
    for j in range(1, chips):
        third[j - 1].wait_recv()
        block = out_ref.at[:, span(core, ahead(chips - j))]
        fourth.append(send(block, block, s4.at[j], r4.at[j], sibling))
    for copy in fourth:
        copy.wait_recv()
    for copy in first + second + third + fourth:
        copy.wait_send()


def shared_stats(total_sum, total_sq, n, channels):
    rows, cols = total_sum.shape
    chips = n // 2
    vmem = pl.BlockSpec(memory_space=pltpu.VMEM)
    counts = (2, chips - 1, chips - 1, chips)
    return pl.pallas_call(
        functools.partial(stats_kernel, n, channels),
        out_shape=jax.ShapeDtypeStruct((2, rows, cols), jnp.float32),
        in_specs=[vmem, vmem],
        out_specs=vmem,
        scratch_shapes=[
            pltpu.VMEM((2, rows // 2, cols), jnp.float32),
            pltpu.VMEM((chips, 2, rows // n, cols), jnp.float32),
            pltpu.VMEM((chips - 1, 2, rows // n, cols), jnp.float32),
        ]
        + [pltpu.SemaphoreType.DMA((c,)) for c in counts for _ in range(2)],
        compiler_params=pltpu.CompilerParams(
            collective_id=0, has_side_effects=True, vmem_limit_bytes=32 * 1024 * 1024
        ),
        name="stats",
    )(total_sum, total_sq)


LANE = 128
SETS = 4


def wave(f, left, right, period):
    return f(
        (left[:, None] * right[None, :] % period).astype(np.float32)
        * np.float32(2.0 * math.pi / period)
    ) * np.float32(1.0 / math.sqrt(period))


def split_tables(rows, cols):
    half_r, half_c = rows // 2, cols // 2
    col, mode = np.arange(half_c), 2 * np.arange(half_c // 2)
    fwd, inv = [], []
    for odd in range(2):
        cos_w, sin_w = (wave(f, col, mode + odd, cols) for f in (np.cos, np.sin))
        fwd.append(np.concatenate([cos_w, -sin_w], axis=1))
        weight = np.where(mode + odd == 0, 1.0, 2.0).astype(np.float32)[:, None]
        inv.append(np.concatenate([cos_w.T * weight, -sin_w.T * weight], axis=0))
    row, pair = np.arange(half_r), 2 * np.arange(rows // 4)
    turn = []
    for odd in range(2):
        cos_h, sin_h = (wave(f, pair + odd, row, rows) for f in (np.cos, np.sin))
        on_re, on_im = [cos_h, -sin_h], [sin_h, cos_h]
        if odd == 0:
            middle = wave(np.cos, np.array([half_r]), row, rows)[0]
            on_re[1][0] = middle
            on_im[0] = on_im[0].copy()
            on_im[0][0] = middle
        for parts in (on_re, on_im):
            blocks = [p.reshape(-1, SETS, half_r) for p in parts]
            turn.append(np.concatenate(blocks, axis=1).reshape(half_r, half_r))
    turn = np.stack(turn)
    tables = (np.stack(fwd), turn, turn.transpose(0, 2, 1), np.stack(inv))
    return tuple(np.ascontiguousarray(t).astype(jnp.bfloat16) for t in tables)


def normal_modes(x_ref, stats_ref, n, scale, fwd_ref, turn_ref, lift):
    rows, cols = x_ref.shape[1:]
    half_r, half_c = rows // 2, cols // 2
    quarter = half_c // 2
    values = x_ref[n].astype(jnp.float32)
    normed = ((values - stats_ref[0]) * stats_ref[1] * scale).astype(jnp.bfloat16)
    left, right = normed[:, :half_c], normed[:, half_c:]
    along = [
        jnp.dot(part, fwd_ref[i], preferred_element_type=jnp.float32).astype(jnp.bfloat16)
        for i, part in enumerate((left + right, left - right))
    ]
    along = [
        jnp.concatenate([a[:, p * quarter : (p + 1) * quarter] for a in along], axis=1)
        for p in range(2)
    ]
    out = []
    for odd in range(2):
        turned = []
        for p in range(2):
            top, low = along[p][:half_r], along[p][half_r:]
            part = top - low if odd else top + low
            turned.append(
                jnp.dot(turn_ref[2 * odd + p], part, preferred_element_type=jnp.float32)
            )
        plus, minus = turned[0] + turned[1], turned[0] - turned[1]
        if odd == 0:
            first, second = turned[0][:SUB], turned[1][:SUB]
            line = lax.broadcasted_iota(jnp.int32, first.shape, 0)
            lane = lax.broadcasted_iota(jnp.int32, first.shape, 1)
            head = jnp.where(line == 0, first, jnp.where(line == SETS, second, plus[:SUB]))
            head = head + jnp.where((line == 0) & (lane == 0), lift, 0.0)
            tail = jnp.where(
                line == 0,
                pltpu.roll(first, SETS, 0),
                jnp.where(line == SETS, -pltpu.roll(second, SETS, 0), minus[:SUB]),
            )
            plus = jnp.concatenate([head, plus[SUB:]], axis=0)
            minus = jnp.concatenate([tail, minus[SUB:]], axis=0)
        out += [plus, minus]
    return out


def wide_weight(real, imag, flip_in, flip_out):
    size = real.shape[0]
    rows = lax.broadcasted_iota(jnp.int32, (size * SUB, size), 0)
    cols = lax.broadcasted_iota(jnp.int32, (size * SUB, size), 1)
    repeat = jnp.where((rows >= cols * SUB) & (rows < cols * SUB + SUB), 1.0, 0.0).astype(
        jnp.bfloat16
    )
    last = (((1,), (1,)), ((), ()))
    full = []
    for weight in (real, imag):
        tall = lax.dot_general(repeat, weight, last, preferred_element_type=jnp.float32)
        full.append(
            lax.dot_general(
                tall.astype(jnp.bfloat16), repeat, last, preferred_element_type=jnp.float32
            )
        )
    left = lax.broadcasted_iota(jnp.int32, full[0].shape, 0)
    right = lax.broadcasted_iota(jnp.int32, full[0].shape, 1)
    same = ((left ^ right) & (SETS - 1)) == 0
    im_out, im_in = (left & SETS) != 0, (right & SETS) != 0
    value = jnp.where(
        im_out, jnp.where(im_in, full[0], full[1]), jnp.where(im_in, -full[1], full[0])
    )
    value = jnp.where(same, value, 0.0)
    flips = []
    for flip_i, flip_o in ((False, False), (flip_in, flip_out)):
        turned = jnp.where(im_in, -value, value) if flip_i else value
        flips.append(jnp.where(im_out, -turned, turned) if flip_o else turned)
    return [f.astype(jnp.bfloat16) for f in flips]


def prepare(block, first_ref, second_ref, bias_ref, w_ref, b1_ref):
    width = first_ref.shape[2]
    size = width * SUB
    for i, (source, flip) in enumerate(((first_ref, True), (second_ref, False))):
        pair = wide_weight(source[0, block], source[1, block], flip, not flip)
        for j in range(2):
            w_ref[2 * i + j] = pair[j]
    shape = (size, bias_ref.shape[1])
    line = lax.broadcasted_iota(jnp.int32, shape, 0)
    offset = line - (lax.broadcasted_iota(jnp.int32, shape, 1) - block * width) * SUB
    own = (offset >= 0) & (offset < SUB)
    picked = jnp.where((line & SETS) == 0, bias_ref[0:1, :], bias_ref[1:2, :])
    column = jnp.sum(jnp.where(own, picked, 0.0), axis=1, keepdims=True)
    b1_ref[...] = jnp.broadcast_to(column, b1_ref.shape)


def mix_pair(a_ref, b_ref, w_ref, b1_ref, odd, start, groups, edge):
    width = b_ref.shape[0]
    cols = b_ref.shape[3]
    sums, gaps = [], []
    for g in range(2):
        mixed = []
        for side in range(2):
            values = a_ref[(2 * odd + side) * groups + start + g]
            hid = jnp.dot(w_ref[side], values, preferred_element_type=jnp.float32)
            hid = (hid + b1_ref[...]).astype(jnp.bfloat16)
            hid = jnp.maximum(hid, jnp.zeros_like(hid))
            out = jnp.dot(w_ref[2 + side], hid, preferred_element_type=jnp.float32)
            mixed.append((out - jnp.clip(out, -0.01, 0.01)).reshape(width, SUB, cols))
        total, gap = mixed[0] + mixed[1], mixed[0] - mixed[1]
        if edge is not None and g == 0:
            line = lax.broadcasted_iota(jnp.int32, total.shape, 1)
            moved = pltpu.roll(mixed[1], SETS, 1)
            re_edge, im_edge = (line == 0) & edge, (line == SETS) & edge
            total = jnp.where(re_edge, mixed[0], jnp.where(im_edge, moved, total))
            gap = jnp.where(re_edge, -moved, jnp.where(im_edge, mixed[0], gap))
        sums.append(total)
        gaps.append(gap)
    spot = pl.ds(pl.multiple_of(start * SUB, 2 * SUB), 2 * SUB)
    for i, parts in enumerate((sums, gaps)):
        b_ref[:, 2 * odd + i, spot, :] = jnp.concatenate(parts, axis=1).astype(jnp.bfloat16)


def return_rows(x_ref, n, b_ref, channel, back_ref, inv_ref, out_ref):
    rows, cols = x_ref.shape[1:]
    half_c = cols // 2
    quarter = half_c // 2
    parts = []
    for p in range(2):
        even, odd = (
            jnp.dot(back_ref[2 * i + p], b_ref[channel, 2 * i + p], preferred_element_type=jnp.float32)
            for i in range(2)
        )
        parts.append(jnp.concatenate([even + odd, even - odd], axis=0).astype(jnp.bfloat16))
    even, odd = (
        jnp.dot(
            jnp.concatenate([t[:, i * quarter : (i + 1) * quarter] for t in parts], axis=1),
            inv_ref[i],
            preferred_element_type=jnp.float32,
        )
        for i in range(2)
    )
    for i, filtered in enumerate((even + odd, even - odd)):
        span = slice(i * half_c, (i + 1) * half_c)
        out_ref[n, :, span] = (x_ref[n, :, span].astype(jnp.float32) + filtered).astype(
            jnp.bfloat16
        )


def main_kernel(
    plan,
    x_ref,
    stats_ref,
    gain_ref,
    shift_ref,
    first_ref,
    second_ref,
    bias_ref,
    fwd_ref,
    turn_ref,
    back_ref,
    inv_ref,
    out_ref,
    a_ref,
    b_ref,
    w_ref,
    b1_ref,
):
    steps, mixes, minis = plan
    step = pl.program_id(0)
    count, rows, cols = x_ref.shape
    half_r = rows // 2
    groups = half_r // SUB
    width = first_ref.shape[2]
    index = lax.axis_index("grid")

    @pl.when(step == 0)
    def _():
        prepare(index, first_ref, second_ref, bias_ref, w_ref, b1_ref)

    @pl.when(step < steps)
    def _():
        here = step * count
        lift_scale = float(cols * rows) * float(fwd_first(cols)) * float(fwd_first(rows))
        for n in range(0, count, 2):
            pair = [
                normal_modes(
                    x_ref,
                    stats_ref,
                    n + i,
                    gain_ref[index * width + here + n + i],
                    fwd_ref,
                    turn_ref,
                    shift_ref[index * width + here + n + i] * lift_scale,
                )
                for i in range(2)
            ]
            spot = pl.ds(pl.multiple_of((here + n) * SUB, 2 * SUB), 2 * SUB)
            for kind in range(4):
                both = [p[kind].reshape(groups, SUB, -1) for p in pair]
                a_ref[kind * groups : (kind + 1) * groups, spot, :] = jnp.concatenate(
                    both, axis=1
                ).astype(jnp.bfloat16)

    @pl.when((step >= steps) & (step < steps + mixes))
    def _():
        now = step - steps
        for u in range(minis):
            mini = now * minis + u
            odd, start = lax.div(mini, groups // 2), 2 * lax.rem(mini, groups // 2)
            mix_pair(
                a_ref, b_ref, w_ref, b1_ref, odd, start, groups, now == 0 if u == 0 else None
            )

    @pl.when(step >= steps + mixes)
    def _():
        here = (step - steps - mixes) * count
        for n in range(count):
            return_rows(x_ref, n, b_ref, here + n, back_ref, inv_ref, out_ref)


def fwd_first(size):
    return np.asarray(np.float32(1.0 / math.sqrt(size))).astype(jnp.bfloat16).astype(np.float32)


def whole_spec(array):
    zeros = (0,) * array.ndim
    return pl.BlockSpec(array.shape, lambda *_: zeros)


def mix_tokens(fields, stats, norm_gain, norm_shift, first_weight, second_weight, first_bias):
    local_ch, rows, cols = fields.shape
    half_r, half_c = rows // 2, cols // 2
    tables = [jnp.asarray(t) for t in split_tables(rows, cols)]
    size = first_weight.shape[2] * SUB
    per = 4 if local_ch % 4 == 0 else 2
    steps = local_ch // per
    minis = 4
    mixes = half_r // SUB // minis
    image = jax.ShapeDtypeStruct(fields.shape, jnp.bfloat16)
    last = steps - 1
    x_spec = pl.BlockSpec(
        (per, rows, cols),
        lambda i: (jnp.where(i < steps, i, jnp.maximum(i - steps - mixes, 0)), 0, 0),
    )
    out_spec = pl.BlockSpec(
        (per, rows, cols), lambda i: (jnp.maximum(i - steps - mixes, 0), 0, 0)
    )
    smem = pl.BlockSpec(memory_space=pltpu.SMEM)
    return pl.pallas_call(
        functools.partial(main_kernel, (steps, mixes, minis)),
        grid=(2 * steps + mixes,),
        out_shape=image,
        in_specs=[x_spec, whole_spec(stats), smem, smem]
        + [whole_spec(t) for t in (first_weight, second_weight, first_bias, *tables)],
        out_specs=out_spec,
        scratch_shapes=[
            pltpu.VMEM((4 * half_r // SUB, size, half_c), jnp.bfloat16),
            pltpu.VMEM((local_ch, 4, half_r, half_c), jnp.bfloat16),
            pltpu.VMEM((4, size, size), jnp.bfloat16),
            pltpu.VMEM((size, half_c), jnp.float32),
        ],
        compiler_params=pltpu.CompilerParams(
            dimension_semantics=("arbitrary",), vmem_limit_bytes=64 * 1000 * 1000
        ),
        cost_estimate=pl.CostEstimate(
            flops=6 * fields.size * rows, bytes_accessed=6 * fields.size, transcendentals=0
        ),
        name="main",
    )(fields, stats, norm_gain, norm_shift, first_weight, second_weight, first_bias, *tables)


def per_device_local(fields, norm_gain, norm_shift, first_weight, second_weight, first_bias):
    groups = lax.axis_size("grid")
    values = fields.astype(jnp.float32)
    stats = shared_stats(
        jnp.sum(values, axis=0),
        jnp.sum(values * values, axis=0),
        groups,
        fields.shape[0] * groups,
    )
    return mix_tokens(
        fields, stats, norm_gain, norm_shift, first_weight, second_weight, first_bias
    )


def per_device_any(fields, norm_gain, norm_shift, first_weight, second_weight, first_bias):
    local_ch, rows, cols = fields.shape
    groups = lax.axis_size("grid")
    one_block = local_ch == first_weight.shape[2] and local_ch % 2 == 0
    tiled = rows % 256 == 0 and cols % 512 == 0 and local_ch * rows * cols <= 8 * 1024 * 1024
    tiled = tiled and groups % 2 == 0 and rows % (8 * groups) == 0
    chosen = per_device_local if one_block and tiled else per_device
    return chosen(fields, norm_gain, norm_shift, first_weight, second_weight, first_bias)


def solution(mesh):
    return jax.shard_map(
        per_device_any,
        mesh=mesh,
        in_specs=(P(("batch", "grid"), None, None), P(), P(), P(), P(), P()),
        out_specs=P(("batch", "grid"), None, None),
        check_vma=False,
    )
```

```python
import functools
import math

import jax
import jax.numpy as jnp
import numpy as np
from jax import lax
from jax.experimental import pallas as pl
from jax.experimental.pallas import tpu as pltpu
from jax.sharding import PartitionSpec as P


def tables(rows, cols):
    half = cols // 2
    col_index = jnp.arange(cols, dtype=jnp.int32)
    mode_index = jnp.arange(half, dtype=jnp.int32)
    angle_w = (col_index[:, None] * mode_index[None, :] % cols).astype(jnp.float32) * (
        2.0 * math.pi / cols
    )
    scale_w = 1.0 / math.sqrt(cols)
    fwd_w = jnp.concatenate(
        [jnp.cos(angle_w) * scale_w, -jnp.sin(angle_w) * scale_w], axis=1
    ).astype(jnp.bfloat16)
    weight_k = jnp.where(mode_index == 0, 1.0, 2.0).astype(jnp.float32)
    inv_w = jnp.concatenate(
        [
            (jnp.cos(angle_w) * weight_k[None, :] * scale_w).T,
            (-jnp.sin(angle_w) * weight_k[None, :] * scale_w).T,
        ],
        axis=0,
    ).astype(jnp.bfloat16)
    row_index = jnp.arange(rows, dtype=jnp.int32)
    angle_h = (row_index[:, None] * row_index[None, :] % rows).astype(jnp.float32) * (
        2.0 * math.pi / rows
    )
    scale_h = 1.0 / math.sqrt(rows)
    cos_h = (jnp.cos(angle_h) * scale_h).astype(jnp.bfloat16)
    sin_h = (jnp.sin(angle_h) * scale_h).astype(jnp.bfloat16)
    return (fwd_w, inv_w, cos_h, sin_h)


def mult(form, left, right):
    return jnp.einsum(form, left, right, preferred_element_type=jnp.float32)


def shrink(values):
    return jnp.maximum(values - 0.01, 0.0) + jnp.minimum(values + 0.01, 0.0)


def mix_modes(real_part, imag_part, first_weight, second_weight, first_bias):
    blocks = first_weight.shape[1]
    width = first_weight.shape[2]
    shape = real_part.shape
    real_blk = real_part.reshape(blocks, width, -1)
    imag_blk = imag_part.reshape(blocks, width, -1)
    bias_blk = first_bias.reshape(2, blocks, width, 1)
    hid_re = jax.nn.relu(
        mult("bio,bim->bom", first_weight[0], real_blk)
        - mult("bio,bim->bom", first_weight[1], imag_blk)
        + bias_blk[0]
    ).astype(jnp.bfloat16)
    hid_im = jax.nn.relu(
        mult("bio,bim->bom", first_weight[0], imag_blk)
        + mult("bio,bim->bom", first_weight[1], real_blk)
        + bias_blk[1]
    ).astype(jnp.bfloat16)
    out_re = mult("bio,bim->bom", second_weight[0], hid_re) - mult(
        "bio,bim->bom", second_weight[1], hid_im
    )
    out_im = mult("bio,bim->bom", second_weight[0], hid_im) + mult(
        "bio,bim->bom", second_weight[1], hid_re
    )
    return (
        shrink(out_re).astype(jnp.bfloat16).reshape(shape),
        shrink(out_im).astype(jnp.bfloat16).reshape(shape),
    )


def per_device(fields, norm_gain, norm_shift, first_weight, second_weight, first_bias):
    local_ch, rows, cols = fields.shape
    half = cols // 2
    groups = lax.axis_size("grid")
    channels = local_ch * groups
    fwd_w, inv_w, cos_h, sin_h = tables(rows, cols)
    values = fields.astype(jnp.float32)
    start = lax.axis_index("grid") * local_ch
    gain_own = lax.dynamic_slice_in_dim(norm_gain, start, local_ch)
    shift_own = lax.dynamic_slice_in_dim(norm_shift, start, local_ch)
    total_sum, total_sq = lax.psum(
        (jnp.sum(values, axis=0), jnp.sum(values * values, axis=0)), "grid"
    )
    mean = total_sum / channels
    var = total_sq / channels - mean * mean
    normed = (
        (values - mean) * lax.rsqrt(var + 1e-05) * gain_own[:, None, None]
        + shift_own[:, None, None]
    ).astype(jnp.bfloat16)
    along_w = (
        mult("chw,wk->chk", normed, fwd_w).astype(jnp.bfloat16).reshape(local_ch, rows, 2, half)
    )
    first_p = mult("kh,chpq->ckpq", cos_h, along_w)
    first_q = mult("kh,chpq->ckpq", sin_h, along_w)
    modes = jnp.stack(
        [
            (first_p[:, :, 0] + first_q[:, :, 1]).astype(jnp.bfloat16),
            (first_p[:, :, 1] - first_q[:, :, 0]).astype(jnp.bfloat16),
        ],
        axis=2,
    )
    spread = lax.all_to_all(modes, "grid", split_axis=1, concat_axis=0, tiled=True)
    shr_re, shr_im = mix_modes(
        spread[:, :, 0], spread[:, :, 1], first_weight, second_weight, first_bias
    )
    gathered = lax.all_to_all(
        jnp.stack([shr_re, shr_im], axis=2), "grid", split_axis=0, concat_axis=1, tiled=True
    )
    back_p = mult("kh,ckpq->chpq", cos_h, gathered)
    back_q = mult("kh,ckpq->chpq", sin_h, gathered)
    back_re = (back_p[:, :, 0] - back_q[:, :, 1]).astype(jnp.bfloat16)
    back_im = (back_p[:, :, 1] + back_q[:, :, 0]).astype(jnp.bfloat16)
    backed = jnp.concatenate([back_re, back_im], axis=2)
    filtered = mult("chk,kw->chw", backed, inv_w)
    return (values + filtered).astype(jnp.bfloat16)

SUB = 8


LANE = 128
SETS = 4


def wave(f, left, right, period):
    return f(
        (left[:, None] * right[None, :] % period).astype(np.float32)
        * np.float32(2.0 * math.pi / period)
    ) * np.float32(1.0 / math.sqrt(period))


def split_tables(rows, cols):
    half_r, half_c = rows // 2, cols // 2
    col, mode = np.arange(half_c), 2 * np.arange(half_c // 2)
    fwd, inv = [], []
    for odd in range(2):
        cos_w, sin_w = (wave(f, col, mode + odd, cols) for f in (np.cos, np.sin))
        fwd.append(np.concatenate([cos_w, -sin_w], axis=1))
        weight = np.where(mode + odd == 0, 1.0, 2.0).astype(np.float32)[:, None]
        inv.append(np.concatenate([cos_w.T * weight, -sin_w.T * weight], axis=0))
    row, pair = np.arange(half_r), 2 * np.arange(rows // 4)
    turn = []
    for odd in range(2):
        cos_h, sin_h = (wave(f, pair + odd, row, rows) for f in (np.cos, np.sin))
        on_re, on_im = [cos_h, -sin_h], [sin_h, cos_h]
        if odd == 0:
            middle = wave(np.cos, np.array([half_r]), row, rows)[0]
            on_re[1][0] = middle
            on_im[0] = on_im[0].copy()
            on_im[0][0] = middle
        for parts in (on_re, on_im):
            blocks = [p.reshape(-1, SETS, half_r) for p in parts]
            turn.append(np.concatenate(blocks, axis=1).reshape(half_r, half_r))
    turn = np.stack(turn)
    tables = (np.stack(fwd), turn, turn.transpose(0, 2, 1), np.stack(inv))
    return tuple(np.ascontiguousarray(t).astype(jnp.bfloat16) for t in tables)


def turn_rows(along_ref, n, turn_ref, lift):
    rows, cols = along_ref.shape[1:]
    half_r, half_c = rows // 2, cols // 2
    quarter = half_c // 2
    along = [
        jnp.concatenate(
            [
                along_ref[n, :, i * half_c + p * quarter : i * half_c + (p + 1) * quarter]
                for i in range(2)
            ],
            axis=1,
        )
        for p in range(2)
    ]
    out = []
    for odd in range(2):
        turned = []
        for p in range(2):
            top, low = along[p][:half_r], along[p][half_r:]
            part = top - low if odd else top + low
            turned.append(
                jnp.dot(turn_ref[2 * odd + p], part, preferred_element_type=jnp.float32)
            )
        plus, minus = turned[0] + turned[1], turned[0] - turned[1]
        if odd == 0:
            first, second = turned[0][:SUB], turned[1][:SUB]
            line = lax.broadcasted_iota(jnp.int32, first.shape, 0)
            lane = lax.broadcasted_iota(jnp.int32, first.shape, 1)
            head = jnp.where(line == 0, first, jnp.where(line == SETS, second, plus[:SUB]))
            head = head + jnp.where((line == 0) & (lane == 0), lift, 0.0)
            tail = jnp.where(
                line == 0,
                pltpu.roll(first, SETS, 0),
                jnp.where(line == SETS, -pltpu.roll(second, SETS, 0), minus[:SUB]),
            )
            plus = jnp.concatenate([head, plus[SUB:]], axis=0)
            minus = jnp.concatenate([tail, minus[SUB:]], axis=0)
        out += [plus, minus]
    return out


def wide_weight(real, imag, flip_in, flip_out):
    size = real.shape[0]
    rows = lax.broadcasted_iota(jnp.int32, (size * SUB, size), 0)
    cols = lax.broadcasted_iota(jnp.int32, (size * SUB, size), 1)
    repeat = jnp.where((rows >= cols * SUB) & (rows < cols * SUB + SUB), 1.0, 0.0).astype(
        jnp.bfloat16
    )
    last = (((1,), (1,)), ((), ()))
    full = []
    for weight in (real, imag):
        tall = lax.dot_general(repeat, weight, last, preferred_element_type=jnp.float32)
        full.append(
            lax.dot_general(
                tall.astype(jnp.bfloat16), repeat, last, preferred_element_type=jnp.float32
            )
        )
    left = lax.broadcasted_iota(jnp.int32, full[0].shape, 0)
    right = lax.broadcasted_iota(jnp.int32, full[0].shape, 1)
    same = ((left ^ right) & (SETS - 1)) == 0
    im_out, im_in = (left & SETS) != 0, (right & SETS) != 0
    value = jnp.where(
        im_out, jnp.where(im_in, full[0], full[1]), jnp.where(im_in, -full[1], full[0])
    )
    value = jnp.where(same, value, 0.0)
    flips = []
    for flip_i, flip_o in ((False, False), (flip_in, flip_out)):
        turned = jnp.where(im_in, -value, value) if flip_i else value
        flips.append(jnp.where(im_out, -turned, turned) if flip_o else turned)
    return [f.astype(jnp.bfloat16) for f in flips]


def prepare(block, first_ref, second_ref, bias_ref, w_ref, b1_ref):
    width = first_ref.shape[2]
    size = width * SUB
    for i, (source, flip) in enumerate(((first_ref, True), (second_ref, False))):
        pair = wide_weight(source[0, block], source[1, block], flip, not flip)
        for j in range(2):
            w_ref[2 * i + j] = pair[j]
    shape = (size, bias_ref.shape[1])
    line = lax.broadcasted_iota(jnp.int32, shape, 0)
    offset = line - (lax.broadcasted_iota(jnp.int32, shape, 1) - block * width) * SUB
    own = (offset >= 0) & (offset < SUB)
    picked = jnp.where((line & SETS) == 0, bias_ref[0:1, :], bias_ref[1:2, :])
    column = jnp.sum(jnp.where(own, picked, 0.0), axis=1, keepdims=True)
    b1_ref[...] = jnp.broadcast_to(column, b1_ref.shape)


CHUNKS = 4
TOGETHER = 4


def token_kernel(
    n,
    x_hbm,
    gain_ref,
    fwd_ref,
    along_hbm,
    x_ref,
    sums,
    stats,
    near,
    part_s,
    part_m,
    far_s,
    far_m,
    ag_out,
    ag_in,
    stage,
    load_sem,
    store_sem,
    s1,
    r1,
    s2,
    r2,
    s3,
    r3,
    s4,
    r4,
):
    me = lax.axis_index("grid")
    chips = n // 2
    core, chip = lax.rem(me, 2), lax.div(me, 2)
    sibling = chip * 2 + 1 - core
    local_ch, rows, cols = x_ref.shape
    half_c = cols // 2
    height = rows // CHUNKS
    half, piece = height // 2, height // n
    share = 2.0 * local_ch

    def ahead(j):
        return lax.rem(chip + j, chips)

    def span(c, owner, k):
        return pl.ds(pl.multiple_of(c * height + owner * half + k * piece, piece), piece)

    def halves(c, owner):
        return pl.ds(pl.multiple_of(c * height + owner * half, half), half)

    def send(source, target, send_sem, recv_sem, device):
        copy = pltpu.make_async_remote_copy(
            src_ref=source,
            dst_ref=target,
            send_sem=send_sem,
            recv_sem=recv_sem,
            device_id={"grid": device},
            device_id_type=pl.DeviceIdType.MESH,
        )
        copy.start()
        return copy

    loads = [
        pltpu.make_async_copy(
            x_hbm.at[:, c * height : (c + 1) * height],
            x_ref.at[:, c * height : (c + 1) * height],
            load_sem.at[c],
        )
        for c in range(CHUNKS)
    ]
    for copy in loads:
        copy.start()
    barrier = pltpu.get_barrier_semaphore()
    for device in [sibling] + [ahead(j) * 2 + core for j in range(1, chips)]:
        pl.semaphore_signal(
            barrier, inc=1, device_id={"grid": device}, device_id_type=pl.DeviceIdType.MESH
        )

    first, second, third, fourth, stores = {}, {}, {}, {}, {}

    def add_local(c):
        loads[c].wait()
        lines = 2 * SUB

        def body(r, carry):
            at = pl.ds(pl.multiple_of(c * height + r * lines, lines), lines)
            total = jnp.zeros((lines, cols), jnp.float32)
            square = jnp.zeros((lines, cols), jnp.float32)
            for ch in range(local_ch):
                value = x_ref[ch, at, :].astype(jnp.float32)
                total = total + value
                square = square + value * value
            sums[0, at, :] = total
            sums[1, at, :] = square
            return carry

        lax.fori_loop(0, height // lines, body, 0)
        if c == 0:
            pl.semaphore_wait(barrier, chips)
        first[c] = send(
            sums.at[:, halves(c, 1 - core)], near.at[c], s1.at[c], r1.at[c], sibling
        )

    def add_chip(c):
        first[c].wait_recv()
        for j in range(1, chips + 1):
            k = ahead(j)
            local = pl.ds(pl.multiple_of(k * piece, piece), piece)
            total = sums[0, span(c, core, k)] + near[c, 0, local]
            square = sums[1, span(c, core, k)] + near[c, 1, local]
            part_s[c, j - 1] = total
            part_m[c, j - 1] = (square - total * total * (1.0 / share)).astype(jnp.bfloat16)
        second[c] = []
        for j in range(1, chips):
            device = ahead(j) * 2 + core
            for i, (source, target) in enumerate(((part_s, far_s), (part_m, far_m))):
                at = (c * (chips - 1) + j - 1) * 2 + i
                second[c].append(
                    send(source.at[c, j - 1], target.at[c, j - 1], s2.at[at], r2.at[at], device)
                )

    def finish(c):
        for copy in second[c]:
            copy.wait_recv()
        own = part_s[c, chips - 1]
        others = [far_s[c, j] for j in range(chips - 1)]
        total = own
        for other in others:
            total = total + other
        mean = total * (1.0 / (share * chips))
        spread = part_m[c, chips - 1].astype(jnp.float32)
        for j in range(chips - 1):
            spread = spread + far_m[c, j].astype(jnp.float32)
        gaps = [mean - other * (1.0 / share) for other in others]
        for gap in gaps + [mean - own * (1.0 / share)]:
            spread = spread + gap * gap * share
        scale = lax.rsqrt(spread * (1.0 / (share * chips)) + 1e-05)
        mine = span(c, core, chip)
        stats[0, mine] = mean
        stats[1, mine] = scale
        third[c] = []
        for j in range(1, chips):
            ag_out[c, j - 1, 0] = gaps[j - 1].astype(jnp.bfloat16)
            ag_out[c, j - 1, 1] = scale.astype(jnp.bfloat16)
        for j in range(1, chips):
            at = c * (chips - 1) + j - 1
            third[c].append(
                send(
                    ag_out.at[c, j - 1],
                    ag_in.at[c, j - 1],
                    s3.at[at],
                    r3.at[at],
                    ahead(chips - j) * 2 + core,
                )
            )

    def collect(c):
        for copy in third[c]:
            copy.wait_recv()
        for j in range(1, chips):
            at = span(c, core, ahead(j))
            gap = ag_in[c, j - 1, 0].astype(jnp.float32)
            stats[0, at] = part_s[c, j - 1] * (1.0 / share) + gap
            stats[1, at] = ag_in[c, j - 1, 1].astype(jnp.float32)
        block = stats.at[:, halves(c, core)]
        fourth[c] = send(block, block, s4.at[c], r4.at[c], sibling)

    def transform(c):
        fourth[c].wait_recv()
        slot = c % 2
        if c >= 2:
            stores[c - 2].wait()
        at = slice(c * height, (c + 1) * height)

        def body(i, carry):
            sides = [[], []]
            for u in range(TOGETHER):
                ch = i * TOGETHER + u
                value = x_ref[ch, at, :].astype(jnp.float32)
                gain = gain_ref[me * local_ch + ch]
                normed = ((value - stats[0, at, :]) * stats[1, at, :] * gain).astype(
                    jnp.bfloat16
                )
                left, right = normed[:, :half_c], normed[:, half_c:]
                sides[0].append(left + right)
                sides[1].append(left - right)
            for side in range(2):
                along = jnp.dot(
                    jnp.concatenate(sides[side], axis=0),
                    fwd_ref[side],
                    preferred_element_type=jnp.float32,
                )
                stage[
                    slot, pl.ds(i * TOGETHER, TOGETHER), :, side * half_c : (side + 1) * half_c
                ] = along.reshape(TOGETHER, height, half_c).astype(jnp.bfloat16)
            return carry

        lax.fori_loop(0, local_ch // TOGETHER, body, 0)
        stores[c] = pltpu.make_async_copy(
            stage.at[slot], along_hbm.at[:, at], store_sem.at[slot]
        )
        stores[c].start()

    stages = (add_local, add_chip, finish, collect, transform)
    for tick in range(CHUNKS + len(stages) - 1):
        for depth, stage_of in enumerate(stages):
            if 0 <= tick - depth < CHUNKS:
                stage_of(tick - depth)
    for c in range(max(CHUNKS - 2, 0), CHUNKS):
        stores[c].wait()
    for c in range(CHUNKS):
        for copy in [first[c], fourth[c]] + second[c] + third[c]:
            copy.wait_send()


def token_rows(fields, norm_gain, fwd, n):
    local_ch, rows, cols = fields.shape
    chips = n // 2
    height = rows // CHUNKS
    half, piece = height // 2, height // n
    counts = (CHUNKS, CHUNKS * (chips - 1) * 2, CHUNKS * (chips - 1), CHUNKS)
    f32, bf16 = jnp.float32, jnp.bfloat16
    return pl.pallas_call(
        functools.partial(token_kernel, n),
        out_shape=jax.ShapeDtypeStruct(fields.shape, bf16),
        in_specs=[
            pl.BlockSpec(memory_space=pl.ANY),
            pl.BlockSpec(memory_space=pltpu.SMEM),
            pl.BlockSpec(memory_space=pltpu.VMEM),
        ],
        out_specs=pl.BlockSpec(memory_space=pl.ANY),
        scratch_shapes=[
            pltpu.VMEM(fields.shape, bf16),
            pltpu.VMEM((2, rows, cols), f32),
            pltpu.VMEM((2, rows, cols), f32),
            pltpu.VMEM((CHUNKS, 2, half, cols), f32),
            pltpu.VMEM((CHUNKS, chips, piece, cols), f32),
            pltpu.VMEM((CHUNKS, chips, piece, cols), bf16),
            pltpu.VMEM((CHUNKS, chips - 1, piece, cols), f32),
            pltpu.VMEM((CHUNKS, chips - 1, piece, cols), bf16),
            pltpu.VMEM((CHUNKS, chips - 1, 2, piece, cols), bf16),
            pltpu.VMEM((CHUNKS, chips - 1, 2, piece, cols), bf16),
            pltpu.VMEM((2, local_ch, height, cols), bf16),
            pltpu.SemaphoreType.DMA((CHUNKS,)),
            pltpu.SemaphoreType.DMA((2,)),
        ]
        + [pltpu.SemaphoreType.DMA((c,)) for c in counts for _ in range(2)],
        compiler_params=pltpu.CompilerParams(
            collective_id=0, has_side_effects=True, vmem_limit_bytes=60 * 1000 * 1000
        ),
        name="tokens",
    )(fields, norm_gain, fwd)


def mix_pair(a_ref, b_ref, w_ref, b1_ref, odd, start, groups, edge):
    width = b_ref.shape[0]
    cols = b_ref.shape[3]
    sums, gaps = [], []
    for g in range(2):
        mixed = []
        for side in range(2):
            values = a_ref[(2 * odd + side) * groups + start + g]
            hid = jnp.dot(w_ref[side], values, preferred_element_type=jnp.float32)
            hid = (hid + b1_ref[...]).astype(jnp.bfloat16)
            hid = jnp.maximum(hid, jnp.zeros_like(hid))
            out = jnp.dot(w_ref[2 + side], hid, preferred_element_type=jnp.float32)
            mixed.append((out - jnp.clip(out, -0.01, 0.01)).reshape(width, SUB, cols))
        total, gap = mixed[0] + mixed[1], mixed[0] - mixed[1]
        if edge is not None and g == 0:
            line = lax.broadcasted_iota(jnp.int32, total.shape, 1)
            moved = pltpu.roll(mixed[1], SETS, 1)
            re_edge, im_edge = (line == 0) & edge, (line == SETS) & edge
            total = jnp.where(re_edge, mixed[0], jnp.where(im_edge, moved, total))
            gap = jnp.where(re_edge, -moved, jnp.where(im_edge, mixed[0], gap))
        sums.append(total)
        gaps.append(gap)
    spot = pl.ds(pl.multiple_of(start * SUB, 2 * SUB), 2 * SUB)
    for i, parts in enumerate((sums, gaps)):
        b_ref[:, 2 * odd + i, spot, :] = jnp.concatenate(parts, axis=1).astype(jnp.bfloat16)


def return_rows(x_ref, n, b_ref, channel, back_ref, inv_ref, out_ref):
    rows, cols = x_ref.shape[1:]
    half_c = cols // 2
    quarter = half_c // 2
    parts = []
    for p in range(2):
        even, odd = (
            jnp.dot(back_ref[2 * i + p], b_ref[channel, 2 * i + p], preferred_element_type=jnp.float32)
            for i in range(2)
        )
        parts.append(jnp.concatenate([even + odd, even - odd], axis=0).astype(jnp.bfloat16))
    even, odd = (
        jnp.dot(
            jnp.concatenate([t[:, i * quarter : (i + 1) * quarter] for t in parts], axis=1),
            inv_ref[i],
            preferred_element_type=jnp.float32,
        )
        for i in range(2)
    )
    for i, filtered in enumerate((even + odd, even - odd)):
        span = slice(i * half_c, (i + 1) * half_c)
        out_ref[n, :, span] = (x_ref[n, :, span].astype(jnp.float32) + filtered).astype(
            jnp.bfloat16
        )


def main_kernel(
    plan,
    x_ref,
    along_ref,
    shift_ref,
    first_ref,
    second_ref,
    bias_ref,
    turn_ref,
    back_ref,
    inv_ref,
    out_ref,
    a_ref,
    b_ref,
    w_ref,
    b1_ref,
):
    steps, mixes, minis = plan
    step = pl.program_id(0)
    count, rows, cols = x_ref.shape
    half_r = rows // 2
    groups = half_r // SUB
    width = first_ref.shape[2]
    index = lax.axis_index("grid")

    @pl.when(step == 0)
    def _():
        prepare(index, first_ref, second_ref, bias_ref, w_ref, b1_ref)

    @pl.when(step < steps)
    def _():
        here = step * count
        lift_scale = float(cols * rows) * float(fwd_first(cols)) * float(fwd_first(rows))
        for n in range(0, count, 2):
            pair = [
                turn_rows(
                    along_ref,
                    n + i,
                    turn_ref,
                    shift_ref[index * width + here + n + i] * lift_scale,
                )
                for i in range(2)
            ]
            spot = pl.ds(pl.multiple_of((here + n) * SUB, 2 * SUB), 2 * SUB)
            for kind in range(4):
                both = [p[kind].reshape(groups, SUB, -1) for p in pair]
                a_ref[kind * groups : (kind + 1) * groups, spot, :] = jnp.concatenate(
                    both, axis=1
                ).astype(jnp.bfloat16)

    @pl.when((step >= steps) & (step < steps + mixes))
    def _():
        now = step - steps
        for u in range(minis):
            mini = now * minis + u
            odd, start = lax.div(mini, groups // 2), 2 * lax.rem(mini, groups // 2)
            mix_pair(
                a_ref, b_ref, w_ref, b1_ref, odd, start, groups, now == 0 if u == 0 else None
            )

    @pl.when(step >= steps + mixes)
    def _():
        here = (step - steps - mixes) * count
        for n in range(count):
            return_rows(x_ref, n, b_ref, here + n, back_ref, inv_ref, out_ref)


def fwd_first(size):
    return np.asarray(np.float32(1.0 / math.sqrt(size))).astype(jnp.bfloat16).astype(np.float32)


def whole_spec(array):
    zeros = (0,) * array.ndim
    return pl.BlockSpec(array.shape, lambda *_: zeros)


def per_device_local(fields, norm_gain, norm_shift, first_weight, second_weight, first_bias):
    local_ch, rows, cols = fields.shape
    half_r, half_c = rows // 2, cols // 2
    fwd, *tables = (jnp.asarray(t) for t in split_tables(rows, cols))
    along = token_rows(fields, norm_gain, fwd, lax.axis_size("grid"))
    size = first_weight.shape[2] * SUB
    per = 4 if local_ch % 4 == 0 else 2
    steps = local_ch // per
    minis = 4
    mixes = half_r // SUB // minis
    image = jax.ShapeDtypeStruct(fields.shape, jnp.bfloat16)
    last = steps - 1
    block = (per, rows, cols)
    along_spec = pl.BlockSpec(block, lambda i: (jnp.minimum(i, last), 0, 0))
    late_spec = pl.BlockSpec(block, lambda i: (jnp.maximum(i - steps - mixes, 0), 0, 0))
    smem = pl.BlockSpec(memory_space=pltpu.SMEM)
    return pl.pallas_call(
        functools.partial(main_kernel, (steps, mixes, minis)),
        grid=(2 * steps + mixes,),
        out_shape=image,
        in_specs=[late_spec, along_spec, smem]
        + [whole_spec(t) for t in (first_weight, second_weight, first_bias, *tables)],
        out_specs=late_spec,
        scratch_shapes=[
            pltpu.VMEM((4 * half_r // SUB, size, half_c), jnp.bfloat16),
            pltpu.VMEM((local_ch, 4, half_r, half_c), jnp.bfloat16),
            pltpu.VMEM((4, size, size), jnp.bfloat16),
            pltpu.VMEM((size, half_c), jnp.float32),
        ],
        compiler_params=pltpu.CompilerParams(
            dimension_semantics=("arbitrary",), vmem_limit_bytes=64 * 1000 * 1000
        ),
        cost_estimate=pl.CostEstimate(
            flops=6 * fields.size * rows, bytes_accessed=6 * fields.size, transcendentals=0
        ),
        name="main",
    )(fields, along, norm_shift, first_weight, second_weight, first_bias, *tables)


def per_device_any(fields, norm_gain, norm_shift, first_weight, second_weight, first_bias):
    local_ch, rows, cols = fields.shape
    groups = lax.axis_size("grid")
    one_block = local_ch == first_weight.shape[2] and local_ch % TOGETHER == 0
    tiled = rows % 256 == 0 and cols % 512 == 0 and local_ch * rows * cols <= 8 * 1024 * 1024
    tiled = tiled and groups % 2 == 0 and groups >= 4 and rows % (64 * groups) == 0
    chosen = per_device_local if one_block and tiled else per_device
    return chosen(fields, norm_gain, norm_shift, first_weight, second_weight, first_bias)


def solution(mesh):
    return jax.shard_map(
        per_device_any,
        mesh=mesh,
        in_specs=(P(("batch", "grid"), None, None), P(), P(), P(), P(), P()),
        out_specs=P(("batch", "grid"), None, None),
        check_vma=False,
    )
```

```python
import functools
import math

import jax
import jax.numpy as jnp
import numpy as np
from jax import lax
from jax.experimental import pallas as pl
from jax.experimental.pallas import tpu as pltpu
from jax.sharding import PartitionSpec as P


def tables(rows, cols):
    half = cols // 2
    col_index = jnp.arange(cols, dtype=jnp.int32)
    mode_index = jnp.arange(half, dtype=jnp.int32)
    angle_w = (col_index[:, None] * mode_index[None, :] % cols).astype(jnp.float32) * (
        2.0 * math.pi / cols
    )
    scale_w = 1.0 / math.sqrt(cols)
    fwd_w = jnp.concatenate(
        [jnp.cos(angle_w) * scale_w, -jnp.sin(angle_w) * scale_w], axis=1
    ).astype(jnp.bfloat16)
    weight_k = jnp.where(mode_index == 0, 1.0, 2.0).astype(jnp.float32)
    inv_w = jnp.concatenate(
        [
            (jnp.cos(angle_w) * weight_k[None, :] * scale_w).T,
            (-jnp.sin(angle_w) * weight_k[None, :] * scale_w).T,
        ],
        axis=0,
    ).astype(jnp.bfloat16)
    row_index = jnp.arange(rows, dtype=jnp.int32)
    angle_h = (row_index[:, None] * row_index[None, :] % rows).astype(jnp.float32) * (
        2.0 * math.pi / rows
    )
    scale_h = 1.0 / math.sqrt(rows)
    cos_h = (jnp.cos(angle_h) * scale_h).astype(jnp.bfloat16)
    sin_h = (jnp.sin(angle_h) * scale_h).astype(jnp.bfloat16)
    return (fwd_w, inv_w, cos_h, sin_h)


def mult(form, left, right):
    return jnp.einsum(form, left, right, preferred_element_type=jnp.float32)


def shrink(values):
    return jnp.maximum(values - 0.01, 0.0) + jnp.minimum(values + 0.01, 0.0)


def mix_modes(real_part, imag_part, first_weight, second_weight, first_bias):
    blocks = first_weight.shape[1]
    width = first_weight.shape[2]
    shape = real_part.shape
    real_blk = real_part.reshape(blocks, width, -1)
    imag_blk = imag_part.reshape(blocks, width, -1)
    bias_blk = first_bias.reshape(2, blocks, width, 1)
    hid_re = jax.nn.relu(
        mult("bio,bim->bom", first_weight[0], real_blk)
        - mult("bio,bim->bom", first_weight[1], imag_blk)
        + bias_blk[0]
    ).astype(jnp.bfloat16)
    hid_im = jax.nn.relu(
        mult("bio,bim->bom", first_weight[0], imag_blk)
        + mult("bio,bim->bom", first_weight[1], real_blk)
        + bias_blk[1]
    ).astype(jnp.bfloat16)
    out_re = mult("bio,bim->bom", second_weight[0], hid_re) - mult(
        "bio,bim->bom", second_weight[1], hid_im
    )
    out_im = mult("bio,bim->bom", second_weight[0], hid_im) + mult(
        "bio,bim->bom", second_weight[1], hid_re
    )
    return (
        shrink(out_re).astype(jnp.bfloat16).reshape(shape),
        shrink(out_im).astype(jnp.bfloat16).reshape(shape),
    )


def per_device(fields, norm_gain, norm_shift, first_weight, second_weight, first_bias):
    local_ch, rows, cols = fields.shape
    half = cols // 2
    groups = lax.axis_size("grid")
    channels = local_ch * groups
    fwd_w, inv_w, cos_h, sin_h = tables(rows, cols)
    values = fields.astype(jnp.float32)
    start = lax.axis_index("grid") * local_ch
    gain_own = lax.dynamic_slice_in_dim(norm_gain, start, local_ch)
    shift_own = lax.dynamic_slice_in_dim(norm_shift, start, local_ch)
    total_sum, total_sq = lax.psum(
        (jnp.sum(values, axis=0), jnp.sum(values * values, axis=0)), "grid"
    )
    mean = total_sum / channels
    var = total_sq / channels - mean * mean
    normed = (
        (values - mean) * lax.rsqrt(var + 1e-05) * gain_own[:, None, None]
        + shift_own[:, None, None]
    ).astype(jnp.bfloat16)
    along_w = (
        mult("chw,wk->chk", normed, fwd_w).astype(jnp.bfloat16).reshape(local_ch, rows, 2, half)
    )
    first_p = mult("kh,chpq->ckpq", cos_h, along_w)
    first_q = mult("kh,chpq->ckpq", sin_h, along_w)
    modes = jnp.stack(
        [
            (first_p[:, :, 0] + first_q[:, :, 1]).astype(jnp.bfloat16),
            (first_p[:, :, 1] - first_q[:, :, 0]).astype(jnp.bfloat16),
        ],
        axis=2,
    )
    spread = lax.all_to_all(modes, "grid", split_axis=1, concat_axis=0, tiled=True)
    shr_re, shr_im = mix_modes(
        spread[:, :, 0], spread[:, :, 1], first_weight, second_weight, first_bias
    )
    gathered = lax.all_to_all(
        jnp.stack([shr_re, shr_im], axis=2), "grid", split_axis=0, concat_axis=1, tiled=True
    )
    back_p = mult("kh,ckpq->chpq", cos_h, gathered)
    back_q = mult("kh,ckpq->chpq", sin_h, gathered)
    back_re = (back_p[:, :, 0] - back_q[:, :, 1]).astype(jnp.bfloat16)
    back_im = (back_p[:, :, 1] + back_q[:, :, 0]).astype(jnp.bfloat16)
    backed = jnp.concatenate([back_re, back_im], axis=2)
    filtered = mult("chk,kw->chw", backed, inv_w)
    return (values + filtered).astype(jnp.bfloat16)

SUB = 8


LANE = 128
SETS = 4


def wave(f, left, right, period):
    return f(
        (left[:, None] * right[None, :] % period).astype(np.float32)
        * np.float32(2.0 * math.pi / period)
    ) * np.float32(1.0 / math.sqrt(period))


def split_tables(rows, cols):
    half_r, half_c = rows // 2, cols // 2
    col, mode = np.arange(half_c), 2 * np.arange(half_c // 2)
    fwd, inv = [], []
    for odd in range(2):
        cos_w, sin_w = (wave(f, col, mode + odd, cols) for f in (np.cos, np.sin))
        fwd.append(np.concatenate([cos_w, -sin_w], axis=1))
        weight = np.where(mode + odd == 0, 1.0, 2.0).astype(np.float32)[:, None]
        inv.append(np.concatenate([cos_w.T * weight, -sin_w.T * weight], axis=0))
    row, pair = np.arange(half_r), 2 * np.arange(rows // 4)
    turn = []
    for odd in range(2):
        cos_h, sin_h = (wave(f, pair + odd, row, rows) for f in (np.cos, np.sin))
        on_re, on_im = [cos_h, -sin_h], [sin_h, cos_h]
        if odd == 0:
            middle = wave(np.cos, np.array([half_r]), row, rows)[0]
            on_re[1][0] = middle
            on_im[0] = on_im[0].copy()
            on_im[0][0] = middle
        for parts in (on_re, on_im):
            blocks = [p.reshape(-1, SETS, half_r) for p in parts]
            turn.append(np.concatenate(blocks, axis=1).reshape(half_r, half_r))
    turn = np.stack(turn)
    tables = (np.stack(fwd), turn, turn.transpose(0, 2, 1), np.stack(inv))
    return tuple(np.ascontiguousarray(t).astype(jnp.bfloat16) for t in tables)


def turn_rows(along_ref, n, turn_ref, lift):
    rows, cols = along_ref.shape[1:]
    half_r, half_c = rows // 2, cols // 2
    quarter = half_c // 2
    along = [
        jnp.concatenate(
            [
                along_ref[n, :, i * half_c + p * quarter : i * half_c + (p + 1) * quarter]
                for i in range(2)
            ],
            axis=1,
        )
        for p in range(2)
    ]
    out = []
    for odd in range(2):
        turned = []
        for p in range(2):
            top, low = along[p][:half_r], along[p][half_r:]
            part = top - low if odd else top + low
            turned.append(
                jnp.dot(turn_ref[2 * odd + p], part, preferred_element_type=jnp.float32)
            )
        plus, minus = turned[0] + turned[1], turned[0] - turned[1]
        if odd == 0:
            first, second = turned[0][:SUB], turned[1][:SUB]
            line = lax.broadcasted_iota(jnp.int32, first.shape, 0)
            lane = lax.broadcasted_iota(jnp.int32, first.shape, 1)
            head = jnp.where(line == 0, first, jnp.where(line == SETS, second, plus[:SUB]))
            head = head + jnp.where((line == 0) & (lane == 0), lift, 0.0)
            tail = jnp.where(
                line == 0,
                pltpu.roll(first, SETS, 0),
                jnp.where(line == SETS, -pltpu.roll(second, SETS, 0), minus[:SUB]),
            )
            plus = jnp.concatenate([head, plus[SUB:]], axis=0)
            minus = jnp.concatenate([tail, minus[SUB:]], axis=0)
        out += [plus, minus]
    return out


def wide_weight(real, imag, flip_in, flip_out):
    size = real.shape[0]
    rows = lax.broadcasted_iota(jnp.int32, (size * SUB, size), 0)
    cols = lax.broadcasted_iota(jnp.int32, (size * SUB, size), 1)
    repeat = jnp.where((rows >= cols * SUB) & (rows < cols * SUB + SUB), 1.0, 0.0).astype(
        jnp.bfloat16
    )
    last = (((1,), (1,)), ((), ()))
    full = []
    for weight in (real, imag):
        tall = lax.dot_general(repeat, weight, last, preferred_element_type=jnp.float32)
        full.append(
            lax.dot_general(
                tall.astype(jnp.bfloat16), repeat, last, preferred_element_type=jnp.float32
            )
        )
    left = lax.broadcasted_iota(jnp.int32, full[0].shape, 0)
    right = lax.broadcasted_iota(jnp.int32, full[0].shape, 1)
    same = ((left ^ right) & (SETS - 1)) == 0
    im_out, im_in = (left & SETS) != 0, (right & SETS) != 0
    value = jnp.where(
        im_out, jnp.where(im_in, full[0], full[1]), jnp.where(im_in, -full[1], full[0])
    )
    value = jnp.where(same, value, 0.0)
    flips = []
    for flip_i, flip_o in ((False, False), (flip_in, flip_out)):
        turned = jnp.where(im_in, -value, value) if flip_i else value
        flips.append(jnp.where(im_out, -turned, turned) if flip_o else turned)
    return [f.astype(jnp.bfloat16) for f in flips]


def prepare(block, first_ref, second_ref, bias_ref, w_ref, b1_ref):
    width = first_ref.shape[2]
    size = width * SUB
    for i, (source, flip) in enumerate(((first_ref, True), (second_ref, False))):
        pair = wide_weight(source[0, block], source[1, block], flip, not flip)
        for j in range(2):
            w_ref[2 * i + j] = pair[j]
    shape = (size, bias_ref.shape[1])
    line = lax.broadcasted_iota(jnp.int32, shape, 0)
    offset = line - (lax.broadcasted_iota(jnp.int32, shape, 1) - block * width) * SUB
    own = (offset >= 0) & (offset < SUB)
    picked = jnp.where((line & SETS) == 0, bias_ref[0:1, :], bias_ref[1:2, :])
    column = jnp.sum(jnp.where(own, picked, 0.0), axis=1, keepdims=True)
    b1_ref[...] = jnp.broadcast_to(column, b1_ref.shape)


CHUNKS = 4
STARTS = (0, 1, 2, 3, 4)
TOGETHER = 4


def token_kernel(
    n,
    x_hbm,
    gain_ref,
    fwd_ref,
    x_ref,
    along_ref,
    sums,
    stats,
    near,
    part_s,
    part_m,
    far_s,
    far_m,
    ag_out,
    ag_in,
    load_sem,
    s1,
    r1,
    s2,
    r2,
    s3,
    r3,
    s4,
    r4,
):
    me = lax.axis_index("grid")
    chips = n // 2
    core, chip = lax.rem(me, 2), lax.div(me, 2)
    sibling = chip * 2 + 1 - core
    local_ch, rows, cols = x_ref.shape
    half_c = cols // 2
    height = rows // CHUNKS
    half, piece = height // 2, height // n
    share = 2.0 * local_ch

    def ahead(j):
        return lax.rem(chip + j, chips)

    def span(c, owner, k):
        return pl.ds(pl.multiple_of(c * height + owner * half + k * piece, piece), piece)

    def halves(c, owner):
        return pl.ds(pl.multiple_of(c * height + owner * half, half), half)

    def send(source, target, send_sem, recv_sem, device):
        copy = pltpu.make_async_remote_copy(
            src_ref=source,
            dst_ref=target,
            send_sem=send_sem,
            recv_sem=recv_sem,
            device_id={"grid": device},
            device_id_type=pl.DeviceIdType.MESH,
        )
        copy.start()
        return copy

    loads = [
        pltpu.make_async_copy(
            x_hbm.at[:, c * height : (c + 1) * height],
            x_ref.at[:, c * height : (c + 1) * height],
            load_sem.at[c],
        )
        for c in range(CHUNKS)
    ]
    for copy in loads:
        copy.start()
    barrier = pltpu.get_barrier_semaphore()
    for device in [sibling] + [ahead(j) * 2 + core for j in range(1, chips)]:
        pl.semaphore_signal(
            barrier, inc=1, device_id={"grid": device}, device_id_type=pl.DeviceIdType.MESH
        )

    first, second, third, fourth = {}, {}, {}, {}

    def add_local(c):
        loads[c].wait()
        lines = 2 * SUB

        def body(r, carry):
            at = pl.ds(pl.multiple_of(c * height + r * lines, lines), lines)
            total = jnp.zeros((lines, cols), jnp.float32)
            square = jnp.zeros((lines, cols), jnp.float32)
            for ch in range(local_ch):
                value = x_ref[ch, at, :].astype(jnp.float32)
                total = total + value
                square = square + value * value
            sums[0, at, :] = total
            sums[1, at, :] = square
            return carry

        lax.fori_loop(0, height // lines, body, 0)
        if c == 0:
            pl.semaphore_wait(barrier, chips)
        first[c] = send(
            sums.at[:, halves(c, 1 - core)], near.at[c], s1.at[c], r1.at[c], sibling
        )

    def add_chip(c):
        first[c].wait_recv()
        for j in range(1, chips + 1):
            k = ahead(j)
            local = pl.ds(pl.multiple_of(k * piece, piece), piece)
            total = sums[0, span(c, core, k)] + near[c, 0, local]
            square = sums[1, span(c, core, k)] + near[c, 1, local]
            part_s[c, j - 1] = total
            part_m[c, j - 1] = (square - total * total * (1.0 / share)).astype(jnp.bfloat16)
        second[c] = []
        for j in range(1, chips):
            device = ahead(j) * 2 + core
            for i, (source, target) in enumerate(((part_s, far_s), (part_m, far_m))):
                at = (c * (chips - 1) + j - 1) * 2 + i
                second[c].append(
                    send(source.at[c, j - 1], target.at[c, j - 1], s2.at[at], r2.at[at], device)
                )

    def finish(c):
        for copy in second[c]:
            copy.wait_recv()
        own = part_s[c, chips - 1]
        others = [far_s[c, j] for j in range(chips - 1)]
        total = own
        for other in others:
            total = total + other
        mean = total * (1.0 / (share * chips))
        spread = part_m[c, chips - 1].astype(jnp.float32)
        for j in range(chips - 1):
            spread = spread + far_m[c, j].astype(jnp.float32)
        gaps = [mean - other * (1.0 / share) for other in others]
        for gap in gaps + [mean - own * (1.0 / share)]:
            spread = spread + gap * gap * share
        scale = lax.rsqrt(spread * (1.0 / (share * chips)) + 1e-05)
        mine = span(c, core, chip)
        stats[0, mine] = mean
        stats[1, mine] = scale
        third[c] = []
        for j in range(1, chips):
            ag_out[c, j - 1, 0] = gaps[j - 1].astype(jnp.bfloat16)
            ag_out[c, j - 1, 1] = scale.astype(jnp.bfloat16)
        for j in range(1, chips):
            at = c * (chips - 1) + j - 1
            third[c].append(
                send(
                    ag_out.at[c, j - 1],
                    ag_in.at[c, j - 1],
                    s3.at[at],
                    r3.at[at],
                    ahead(chips - j) * 2 + core,
                )
            )

    def collect(c):
        for copy in third[c]:
            copy.wait_recv()
        for j in range(1, chips):
            at = span(c, core, ahead(j))
            gap = ag_in[c, j - 1, 0].astype(jnp.float32)
            stats[0, at] = part_s[c, j - 1] * (1.0 / share) + gap
            stats[1, at] = ag_in[c, j - 1, 1].astype(jnp.float32)
        block = stats.at[:, halves(c, core)]
        fourth[c] = send(block, block, s4.at[c], r4.at[c], sibling)

    def transform(c):
        fourth[c].wait_recv()
        at = slice(c * height, (c + 1) * height)

        def body(i, carry):
            sides = [[], []]
            for u in range(TOGETHER):
                ch = i * TOGETHER + u
                value = x_ref[ch, at, :].astype(jnp.float32)
                gain = gain_ref[me * local_ch + ch]
                normed = ((value - stats[0, at, :]) * stats[1, at, :] * gain).astype(
                    jnp.bfloat16
                )
                left, right = normed[:, :half_c], normed[:, half_c:]
                sides[0].append(left + right)
                sides[1].append(left - right)
            for side in range(2):
                along = jnp.dot(
                    jnp.concatenate(sides[side], axis=0),
                    fwd_ref[side],
                    preferred_element_type=jnp.float32,
                )
                along_ref[
                    pl.ds(i * TOGETHER, TOGETHER), at, side * half_c : (side + 1) * half_c
                ] = along.reshape(TOGETHER, height, half_c).astype(jnp.bfloat16)
            return carry

        lax.fori_loop(0, local_ch // TOGETHER, body, 0)

    stages = (add_local, add_chip, finish, collect, transform)
    for tick in range(CHUNKS + sum(STARTS)):
        for stage_of, start in zip(stages, STARTS):
            if 0 <= tick - start < CHUNKS:
                stage_of(tick - start)
    for c in range(CHUNKS):
        for copy in [first[c], fourth[c]] + second[c] + third[c]:
            copy.wait_send()


def token_rows(fields, norm_gain, fwd, n):
    local_ch, rows, cols = fields.shape
    chips = n // 2
    height = rows // CHUNKS
    half, piece = height // 2, height // n
    counts = (CHUNKS, CHUNKS * (chips - 1) * 2, CHUNKS * (chips - 1), CHUNKS)
    f32, bf16 = jnp.float32, jnp.bfloat16
    return pl.pallas_call(
        functools.partial(token_kernel, n),
        out_shape=[pltpu.VMEM(fields.shape, bf16)] * 2,
        in_specs=[
            pl.BlockSpec(memory_space=pl.ANY),
            pl.BlockSpec(memory_space=pltpu.SMEM),
            pl.BlockSpec(memory_space=pltpu.VMEM),
        ],
        out_specs=[pl.BlockSpec(memory_space=pltpu.VMEM)] * 2,
        scratch_shapes=[
            pltpu.VMEM((2, rows, cols), f32),
            pltpu.VMEM((2, rows, cols), f32),
            pltpu.VMEM((CHUNKS, 2, half, cols), f32),
            pltpu.VMEM((CHUNKS, chips, piece, cols), f32),
            pltpu.VMEM((CHUNKS, chips, piece, cols), bf16),
            pltpu.VMEM((CHUNKS, chips - 1, piece, cols), f32),
            pltpu.VMEM((CHUNKS, chips - 1, piece, cols), bf16),
            pltpu.VMEM((CHUNKS, chips - 1, 2, piece, cols), bf16),
            pltpu.VMEM((CHUNKS, chips - 1, 2, piece, cols), bf16),
            pltpu.SemaphoreType.DMA((CHUNKS,)),
        ]
        + [pltpu.SemaphoreType.DMA((c,)) for c in counts for _ in range(2)],
        compiler_params=pltpu.CompilerParams(
            collective_id=0, has_side_effects=True, vmem_limit_bytes=28 * 1024 * 1024
        ),
        name="tokens",
    )(fields, norm_gain, fwd)


def mix_pair(a_ref, b_ref, w_ref, b1_ref, odd, start, groups, edge):
    width, rows, cols = b_ref.shape
    half_r, half_c = rows // 2, cols // 2
    sums, gaps = [], []
    for g in range(2):
        mixed = []
        for side in range(2):
            values = a_ref[(2 * odd + side) * groups + start + g]
            hid = jnp.dot(w_ref[side], values, preferred_element_type=jnp.float32)
            hid = (hid + b1_ref[...]).astype(jnp.bfloat16)
            hid = jnp.maximum(hid, jnp.zeros_like(hid))
            out = jnp.dot(w_ref[2 + side], hid, preferred_element_type=jnp.float32)
            mixed.append((out - jnp.clip(out, -0.01, 0.01)).reshape(width, SUB, half_c))
        total, gap = mixed[0] + mixed[1], mixed[0] - mixed[1]
        if edge is not None and g == 0:
            line = lax.broadcasted_iota(jnp.int32, total.shape, 1)
            moved = pltpu.roll(mixed[1], SETS, 1)
            re_edge, im_edge = (line == 0) & edge, (line == SETS) & edge
            total = jnp.where(re_edge, mixed[0], jnp.where(im_edge, moved, total))
            gap = jnp.where(re_edge, -moved, jnp.where(im_edge, mixed[0], gap))
        sums.append(total)
        gaps.append(gap)
    spot = pl.ds(pl.multiple_of(odd * half_r + start * SUB, 2 * SUB), 2 * SUB)
    for i, parts in enumerate((sums, gaps)):
        b_ref[:, spot, i * half_c : (i + 1) * half_c] = jnp.concatenate(parts, axis=1).astype(
            jnp.bfloat16
        )


def return_rows(x_ref, b_ref, channel, back_ref, inv_ref, out_ref):
    local_ch, rows, cols = x_ref.shape
    half_r, half_c = rows // 2, cols // 2
    quarter = half_c // 2
    parts = []
    for p in range(2):
        even, odd = (
            jnp.dot(
                back_ref[2 * i + p],
                b_ref[channel, i * half_r : (i + 1) * half_r, p * half_c : (p + 1) * half_c],
                preferred_element_type=jnp.float32,
            )
            for i in range(2)
        )
        parts.append(jnp.concatenate([even + odd, even - odd], axis=0).astype(jnp.bfloat16))
    even, odd = (
        jnp.dot(
            jnp.concatenate([t[:, i * quarter : (i + 1) * quarter] for t in parts], axis=1),
            inv_ref[i],
            preferred_element_type=jnp.float32,
        )
        for i in range(2)
    )
    for i, filtered in enumerate((even + odd, even - odd)):
        span = slice(i * half_c, (i + 1) * half_c)
        for j in range(2):
            line = slice(j * half_r, (j + 1) * half_r)
            out_ref[(2 * j + i) * local_ch + channel] = (
                x_ref[channel, line, span].astype(jnp.float32) + filtered[line]
            ).astype(jnp.bfloat16)


def main_kernel(
    plan,
    x_ref,
    along_in,
    shift_ref,
    first_ref,
    second_ref,
    bias_ref,
    turn_hbm,
    back_hbm,
    inv_hbm,
    out_hbm,
    b_ref,
    a_ref,
    turn_ref,
    back_ref,
    inv_ref,
    w_ref,
    b1_ref,
    store_sem,
    table_sem,
):
    count, minis = plan
    local_ch, rows, cols = x_ref.shape
    steps = local_ch // count
    half_r, half_c = rows // 2, cols // 2
    groups = half_r // SUB
    index = lax.axis_index("grid")
    tables = [
        pltpu.make_async_copy(source, target, table_sem.at[i])
        for i, (source, target) in enumerate(
            ((turn_hbm, turn_ref), (back_hbm, back_ref), (inv_hbm, inv_ref))
        )
    ]

    def result(i):
        at = pl.ds(i * count, count)
        return [
            pltpu.make_async_copy(
                a_ref.at[pl.ds((2 * j + k) * local_ch + i * count, count)],
                out_hbm.at[
                    at, j * half_r : (j + 1) * half_r, k * half_c : (k + 1) * half_c
                ],
                store_sem.at[i * 4 + 2 * j + k],
            )
            for j in range(2)
            for k in range(2)
        ]

    for table in tables:
        table.start()
    prepare(index, first_ref, second_ref, bias_ref, w_ref, b1_ref)
    tables[0].wait()
    lift_scale = float(cols * rows) * float(fwd_first(cols)) * float(fwd_first(rows))

    def forward(i, carry):
        for n in range(0, count, 2):
            here = i * count + n
            pair = [
                turn_rows(
                    b_ref,
                    here + u,
                    turn_ref,
                    shift_ref[index * local_ch + here + u] * lift_scale,
                )
                for u in range(2)
            ]
            spot = pl.ds(pl.multiple_of(here * SUB, 2 * SUB), 2 * SUB)
            for kind in range(4):
                both = [p[kind].reshape(groups, SUB, -1) for p in pair]
                a_ref[kind * groups : (kind + 1) * groups, spot, :] = jnp.concatenate(
                    both, axis=1
                ).astype(jnp.bfloat16)
        return carry

    lax.fori_loop(0, steps, forward, 0)

    def mix(i, carry):
        for u in range(minis):
            mini = i * minis + u
            odd, start = lax.div(mini, groups // 2), 2 * lax.rem(mini, groups // 2)
            mix_pair(
                a_ref, b_ref, w_ref, b1_ref, odd, start, groups, i == 0 if u == 0 else None
            )
        return carry

    lax.fori_loop(0, groups // minis, mix, 0)
    for table in tables[1:]:
        table.wait()

    def backward(i, carry):
        for n in range(count):
            return_rows(x_ref, b_ref, i * count + n, back_ref, inv_ref, a_ref)
        for copy in result(i):
            copy.start()
        return carry

    lax.fori_loop(0, steps, backward, 0)
    for i in range(steps):
        for copy in result(i):
            copy.wait()


def fwd_first(size):
    return np.asarray(np.float32(1.0 / math.sqrt(size))).astype(jnp.bfloat16).astype(np.float32)


def per_device_local(fields, norm_gain, norm_shift, first_weight, second_weight, first_bias):
    local_ch, rows, cols = fields.shape
    half_r, half_c = rows // 2, cols // 2
    fwd, *tables = (jnp.asarray(t) for t in split_tables(rows, cols))
    near = pltpu.VMEM
    kept = [
        pltpu.with_memory_space_constraint(t, near)
        for t in token_rows(fields, norm_gain, fwd, lax.axis_size("grid"))
    ]
    size = first_weight.shape[2] * SUB
    count, minis = 4, 4
    steps = local_ch // count
    smem = pl.BlockSpec(memory_space=pltpu.SMEM)
    far = pl.BlockSpec(memory_space=pl.ANY)
    held = pl.BlockSpec(memory_space=near)
    result, _ = pl.pallas_call(
        functools.partial(main_kernel, (count, minis)),
        out_shape=[jax.ShapeDtypeStruct(fields.shape, jnp.bfloat16)]
        + [near(fields.shape, jnp.bfloat16)],
        in_specs=[held, held, smem, held, held, held, far, far, far],
        out_specs=[far, held],
        input_output_aliases={1: 1},
        scratch_shapes=[
            pltpu.VMEM((4 * half_r // SUB, size, half_c), jnp.bfloat16),
        ]
        + [pltpu.VMEM(t.shape, jnp.bfloat16) for t in tables]
        + [
            pltpu.VMEM((4, size, size), jnp.bfloat16),
            pltpu.VMEM((size, half_c), jnp.float32),
        ]
        + [pltpu.SemaphoreType.DMA((c,)) for c in (4 * steps, 3)],
        compiler_params=pltpu.CompilerParams(vmem_limit_bytes=28 * 1024 * 1024),
        cost_estimate=pl.CostEstimate(
            flops=6 * fields.size * rows, bytes_accessed=6 * fields.size, transcendentals=0
        ),
        name="main",
    )(*kept, norm_shift, first_weight, second_weight, first_bias, *tables)
    return result


def per_device_any(fields, norm_gain, norm_shift, first_weight, second_weight, first_bias):
    local_ch, rows, cols = fields.shape
    groups = lax.axis_size("grid")
    one_block = local_ch == first_weight.shape[2] and local_ch % TOGETHER == 0
    tiled = rows % 256 == 0 and cols % 512 == 0 and local_ch * rows * cols <= 8 * 1024 * 1024
    tiled = tiled and SUB * local_ch == rows // 2 and groups % 2 == 0 and groups >= 4 and rows % (64 * groups) == 0
    chosen = per_device_local if one_block and tiled else per_device
    return chosen(fields, norm_gain, norm_shift, first_weight, second_weight, first_bias)


def solution(mesh):
    return jax.shard_map(
        per_device_any,
        mesh=mesh,
        in_specs=(P(("batch", "grid"), None, None), P(), P(), P(), P(), P()),
        out_specs=P(("batch", "grid"), None, None),
        check_vma=False,
    )
```

```python
import functools
import math

import jax
import jax.numpy as jnp
import numpy as np
from jax import lax
from jax.experimental import pallas as pl
from jax.experimental.pallas import tpu as pltpu
from jax.sharding import PartitionSpec as P


def tables(rows, cols):
    half = cols // 2
    col_index = jnp.arange(cols, dtype=jnp.int32)
    mode_index = jnp.arange(half, dtype=jnp.int32)
    angle_w = (col_index[:, None] * mode_index[None, :] % cols).astype(jnp.float32) * (
        2.0 * math.pi / cols
    )
    scale_w = 1.0 / math.sqrt(cols)
    fwd_w = jnp.concatenate(
        [jnp.cos(angle_w) * scale_w, -jnp.sin(angle_w) * scale_w], axis=1
    ).astype(jnp.bfloat16)
    weight_k = jnp.where(mode_index == 0, 1.0, 2.0).astype(jnp.float32)
    inv_w = jnp.concatenate(
        [
            (jnp.cos(angle_w) * weight_k[None, :] * scale_w).T,
            (-jnp.sin(angle_w) * weight_k[None, :] * scale_w).T,
        ],
        axis=0,
    ).astype(jnp.bfloat16)
    row_index = jnp.arange(rows, dtype=jnp.int32)
    angle_h = (row_index[:, None] * row_index[None, :] % rows).astype(jnp.float32) * (
        2.0 * math.pi / rows
    )
    scale_h = 1.0 / math.sqrt(rows)
    cos_h = (jnp.cos(angle_h) * scale_h).astype(jnp.bfloat16)
    sin_h = (jnp.sin(angle_h) * scale_h).astype(jnp.bfloat16)
    return (fwd_w, inv_w, cos_h, sin_h)


def mult(form, left, right):
    return jnp.einsum(form, left, right, preferred_element_type=jnp.float32)


def shrink(values):
    return jnp.maximum(values - 0.01, 0.0) + jnp.minimum(values + 0.01, 0.0)


def mix_modes(real_part, imag_part, first_weight, second_weight, first_bias):
    blocks = first_weight.shape[1]
    width = first_weight.shape[2]
    shape = real_part.shape
    real_blk = real_part.reshape(blocks, width, -1)
    imag_blk = imag_part.reshape(blocks, width, -1)
    bias_blk = first_bias.reshape(2, blocks, width, 1)
    hid_re = jax.nn.relu(
        mult("bio,bim->bom", first_weight[0], real_blk)
        - mult("bio,bim->bom", first_weight[1], imag_blk)
        + bias_blk[0]
    ).astype(jnp.bfloat16)
    hid_im = jax.nn.relu(
        mult("bio,bim->bom", first_weight[0], imag_blk)
        + mult("bio,bim->bom", first_weight[1], real_blk)
        + bias_blk[1]
    ).astype(jnp.bfloat16)
    out_re = mult("bio,bim->bom", second_weight[0], hid_re) - mult(
        "bio,bim->bom", second_weight[1], hid_im
    )
    out_im = mult("bio,bim->bom", second_weight[0], hid_im) + mult(
        "bio,bim->bom", second_weight[1], hid_re
    )
    return (
        shrink(out_re).astype(jnp.bfloat16).reshape(shape),
        shrink(out_im).astype(jnp.bfloat16).reshape(shape),
    )


def per_device(fields, norm_gain, norm_shift, first_weight, second_weight, first_bias):
    local_ch, rows, cols = fields.shape
    half = cols // 2
    groups = lax.axis_size("grid")
    channels = local_ch * groups
    fwd_w, inv_w, cos_h, sin_h = tables(rows, cols)
    values = fields.astype(jnp.float32)
    start = lax.axis_index("grid") * local_ch
    gain_own = lax.dynamic_slice_in_dim(norm_gain, start, local_ch)
    shift_own = lax.dynamic_slice_in_dim(norm_shift, start, local_ch)
    total_sum, total_sq = lax.psum(
        (jnp.sum(values, axis=0), jnp.sum(values * values, axis=0)), "grid"
    )
    mean = total_sum / channels
    var = total_sq / channels - mean * mean
    normed = (
        (values - mean) * lax.rsqrt(var + 1e-05) * gain_own[:, None, None]
        + shift_own[:, None, None]
    ).astype(jnp.bfloat16)
    along_w = (
        mult("chw,wk->chk", normed, fwd_w).astype(jnp.bfloat16).reshape(local_ch, rows, 2, half)
    )
    first_p = mult("kh,chpq->ckpq", cos_h, along_w)
    first_q = mult("kh,chpq->ckpq", sin_h, along_w)
    modes = jnp.stack(
        [
            (first_p[:, :, 0] + first_q[:, :, 1]).astype(jnp.bfloat16),
            (first_p[:, :, 1] - first_q[:, :, 0]).astype(jnp.bfloat16),
        ],
        axis=2,
    )
    spread = lax.all_to_all(modes, "grid", split_axis=1, concat_axis=0, tiled=True)
    shr_re, shr_im = mix_modes(
        spread[:, :, 0], spread[:, :, 1], first_weight, second_weight, first_bias
    )
    gathered = lax.all_to_all(
        jnp.stack([shr_re, shr_im], axis=2), "grid", split_axis=0, concat_axis=1, tiled=True
    )
    back_p = mult("kh,ckpq->chpq", cos_h, gathered)
    back_q = mult("kh,ckpq->chpq", sin_h, gathered)
    back_re = (back_p[:, :, 0] - back_q[:, :, 1]).astype(jnp.bfloat16)
    back_im = (back_p[:, :, 1] + back_q[:, :, 0]).astype(jnp.bfloat16)
    backed = jnp.concatenate([back_re, back_im], axis=2)
    filtered = mult("chk,kw->chw", backed, inv_w)
    return (values + filtered).astype(jnp.bfloat16)

SUB = 8


LANE = 128
SETS = 4


def wave(f, left, right, period):
    return f(
        (left[:, None] * right[None, :] % period).astype(np.float32)
        * np.float32(2.0 * math.pi / period)
    ) * np.float32(1.0 / math.sqrt(period))


def split_tables(rows, cols):
    half_r, half_c = rows // 2, cols // 2
    col, mode = np.arange(half_c), 2 * np.arange(half_c // 2)
    fwd, inv = [], []
    for odd in range(2):
        cos_w, sin_w = (wave(f, col, mode + odd, cols) for f in (np.cos, np.sin))
        fwd.append(np.concatenate([cos_w, -sin_w], axis=1))
        weight = np.where(mode + odd == 0, 1.0, 2.0).astype(np.float32)[:, None]
        inv.append(np.concatenate([cos_w.T * weight, -sin_w.T * weight], axis=0))
    row, pair = np.arange(half_r), 2 * np.arange(rows // 4)
    turn = []
    for odd in range(2):
        cos_h, sin_h = (wave(f, pair + odd, row, rows) for f in (np.cos, np.sin))
        on_re, on_im = [cos_h, -sin_h], [sin_h, cos_h]
        if odd == 0:
            middle = wave(np.cos, np.array([half_r]), row, rows)[0]
            on_re[1][0] = middle
            on_im[0] = on_im[0].copy()
            on_im[0][0] = middle
        for parts in (on_re, on_im):
            blocks = [p.reshape(-1, SETS, half_r) for p in parts]
            turn.append(np.concatenate(blocks, axis=1).reshape(half_r, half_r))
    turn = np.stack(turn)
    tables = (np.stack(fwd), turn, turn.transpose(0, 2, 1), np.stack(inv))
    return tuple(np.ascontiguousarray(t).astype(jnp.bfloat16) for t in tables)


def turn_rows(along_ref, n, turn_ref, lift):
    rows, cols = along_ref.shape[1:]
    half_r, half_c = rows // 2, cols // 2
    quarter = half_c // 2
    along = [
        jnp.concatenate(
            [
                along_ref[n, :, i * half_c + p * quarter : i * half_c + (p + 1) * quarter]
                for i in range(2)
            ],
            axis=1,
        )
        for p in range(2)
    ]
    out = []
    for odd in range(2):
        turned = []
        for p in range(2):
            top, low = along[p][:half_r], along[p][half_r:]
            part = top - low if odd else top + low
            turned.append(
                jnp.dot(turn_ref[2 * odd + p], part, preferred_element_type=jnp.float32)
            )
        plus, minus = turned[0] + turned[1], turned[0] - turned[1]
        if odd == 0:
            first, second = turned[0][:SUB], turned[1][:SUB]
            line = lax.broadcasted_iota(jnp.int32, first.shape, 0)
            lane = lax.broadcasted_iota(jnp.int32, first.shape, 1)
            head = jnp.where(line == 0, first, jnp.where(line == SETS, second, plus[:SUB]))
            head = head + jnp.where((line == 0) & (lane == 0), lift, 0.0)
            tail = jnp.where(
                line == 0,
                pltpu.roll(first, SETS, 0),
                jnp.where(line == SETS, -pltpu.roll(second, SETS, 0), minus[:SUB]),
            )
            plus = jnp.concatenate([head, plus[SUB:]], axis=0)
            minus = jnp.concatenate([tail, minus[SUB:]], axis=0)
        out += [plus, minus]
    return out


def wide_weight(real, imag, flip_in, flip_out):
    size = real.shape[0]
    rows = lax.broadcasted_iota(jnp.int32, (size * SUB, size), 0)
    cols = lax.broadcasted_iota(jnp.int32, (size * SUB, size), 1)
    repeat = jnp.where((rows >= cols * SUB) & (rows < cols * SUB + SUB), 1.0, 0.0).astype(
        jnp.bfloat16
    )
    last = (((1,), (1,)), ((), ()))
    full = []
    for weight in (real, imag):
        tall = lax.dot_general(repeat, weight, last, preferred_element_type=jnp.float32)
        full.append(
            lax.dot_general(
                tall.astype(jnp.bfloat16), repeat, last, preferred_element_type=jnp.float32
            )
        )
    left = lax.broadcasted_iota(jnp.int32, full[0].shape, 0)
    right = lax.broadcasted_iota(jnp.int32, full[0].shape, 1)
    same = ((left ^ right) & (SETS - 1)) == 0
    im_out, im_in = (left & SETS) != 0, (right & SETS) != 0
    value = jnp.where(
        im_out, jnp.where(im_in, full[0], full[1]), jnp.where(im_in, -full[1], full[0])
    )
    value = jnp.where(same, value, 0.0)
    flips = []
    for flip_i, flip_o in ((False, False), (flip_in, flip_out)):
        turned = jnp.where(im_in, -value, value) if flip_i else value
        flips.append(jnp.where(im_out, -turned, turned) if flip_o else turned)
    return [f.astype(jnp.bfloat16) for f in flips]


def prepare(block, gain_ref, first_ref, second_ref, bias_ref, w_ref, b1_ref):
    width = first_ref.shape[2]
    size = width * SUB
    row = lax.broadcasted_iota(jnp.int32, (width, width), 0)
    gain = jnp.zeros((width, width), jnp.float32)
    for i in range(width):
        gain = jnp.where(row == i, gain_ref[block * width + i], gain)
    for i, (source, flip) in enumerate(((first_ref, True), (second_ref, False))):
        parts = [source[p, block] for p in range(2)]
        if i == 0:
            parts = [(p.astype(jnp.float32) * gain).astype(jnp.bfloat16) for p in parts]
        pair = wide_weight(*parts, flip, not flip)
        for j in range(2):
            w_ref[2 * i + j] = pair[j]
    shape = (size, bias_ref.shape[1])
    line = lax.broadcasted_iota(jnp.int32, shape, 0)
    offset = line - (lax.broadcasted_iota(jnp.int32, shape, 1) - block * width) * SUB
    own = (offset >= 0) & (offset < SUB)
    picked = jnp.where((line & SETS) == 0, bias_ref[0:1, :], bias_ref[1:2, :])
    column = jnp.sum(jnp.where(own, picked, 0.0), axis=1, keepdims=True)
    b1_ref[...] = jnp.broadcast_to(column, b1_ref.shape)


CHUNKS = 4
STARTS = (0, 1, 4, 8, 9)
TOGETHER = 16


def token_kernel(
    n,
    x_hbm,
    fwd_ref,
    x_ref,
    along_ref,
    sums,
    stats,
    near,
    part,
    far,
    ag_out,
    ag_in,
    load_sem,
    s1,
    r1,
    s2,
    r2,
    s3,
    r3,
    s4,
    r4,
):
    me = lax.axis_index("grid")
    chips = n // 2
    core, chip = lax.rem(me, 2), lax.div(me, 2)
    sibling = chip * 2 + 1 - core
    local_ch, rows, cols = x_ref.shape
    half_c = cols // 2
    height = rows // CHUNKS
    half, piece = height // 2, height // n
    share = 2.0 * local_ch

    def ahead(j):
        return lax.rem(chip + j, chips)

    def span(c, owner, k):
        return pl.ds(pl.multiple_of(c * height + owner * half + k * piece, piece), piece)

    def halves(c, owner):
        return pl.ds(pl.multiple_of(c * height + owner * half, half), half)

    def total_of(ref, c, j):
        return ref[c, j, 0].astype(jnp.float32) + ref[c, j, 1].astype(jnp.float32)

    def keep(at, mean, scale):
        high = mean.astype(jnp.bfloat16)
        stats[0, at] = high
        stats[1, at] = (mean - high.astype(jnp.float32)).astype(jnp.bfloat16)
        stats[2, at] = scale

    def send(source, target, send_sem, recv_sem, device):
        copy = pltpu.make_async_remote_copy(
            src_ref=source,
            dst_ref=target,
            send_sem=send_sem,
            recv_sem=recv_sem,
            device_id={"grid": device},
            device_id_type=pl.DeviceIdType.MESH,
        )
        copy.start()
        return copy

    loads = [
        pltpu.make_async_copy(
            x_hbm.at[:, c * height : (c + 1) * height],
            x_ref.at[:, c * height : (c + 1) * height],
            load_sem.at[c],
        )
        for c in range(CHUNKS)
    ]
    for copy in loads:
        copy.start()
    barrier = pltpu.get_barrier_semaphore()
    for device in [sibling] + [ahead(j) * 2 + core for j in range(1, chips)]:
        pl.semaphore_signal(
            barrier, inc=1, device_id={"grid": device}, device_id_type=pl.DeviceIdType.MESH
        )

    first, second, third, fourth = {}, {}, {}, {}

    def add_local(c):
        loads[c].wait()
        lines = 2 * SUB

        def body(r, carry):
            at = pl.ds(pl.multiple_of(c * height + r * lines, lines), lines)
            total = jnp.zeros((lines, cols), jnp.float32)
            square = jnp.zeros((lines, cols), jnp.float32)
            for ch in range(local_ch):
                value = x_ref[ch, at, :].astype(jnp.float32)
                total = total + value
                square = square + value * value
            sums[0, at, :] = total
            sums[1, at, :] = square
            return carry

        lax.fori_loop(0, height // lines, body, 0)
        if c == 0:
            pl.semaphore_wait(barrier, chips)
        first[c] = send(
            sums.at[:, halves(c, 1 - core)], near.at[c], s1.at[c], r1.at[c], sibling
        )

    def add_chip(c):
        first[c].wait_recv()
        for j in range(1, chips + 1):
            k = ahead(j)
            local = pl.ds(pl.multiple_of(k * piece, piece), piece)
            total = sums[0, span(c, core, k)] + near[c, 0, local]
            square = sums[1, span(c, core, k)] + near[c, 1, local]
            high = total.astype(jnp.bfloat16)
            low = (total - high.astype(jnp.float32)).astype(jnp.bfloat16)
            spread = (square - total * total * (1.0 / share)).astype(jnp.bfloat16)
            for i, plane in enumerate((high, low, spread)):
                part[c, j - 1, i] = plane
        second[c] = []
        for j in range(1, chips):
            at = c * (chips - 1) + j - 1
            second[c].append(
                send(
                    part.at[c, j - 1],
                    far.at[c, j - 1],
                    s2.at[at],
                    r2.at[at],
                    ahead(j) * 2 + core,
                )
            )

    def finish(c):
        for copy in second[c]:
            copy.wait_recv()
        own = total_of(part, c, chips - 1)
        others = [total_of(far, c, j) for j in range(chips - 1)]
        total = own
        for other in others:
            total = total + other
        mean = total * (1.0 / (share * chips))
        spread = part[c, chips - 1, 2].astype(jnp.float32)
        for j in range(chips - 1):
            spread = spread + far[c, j, 2].astype(jnp.float32)
        gaps = [mean - other * (1.0 / share) for other in others]
        for gap in gaps + [mean - own * (1.0 / share)]:
            spread = spread + gap * gap * share
        scale = lax.rsqrt(spread * (1.0 / (share * chips)) + 1e-05)
        keep(span(c, core, chip), mean, scale.astype(jnp.bfloat16))
        third[c] = []
        for j in range(1, chips):
            ag_out[c, j - 1, 0] = gaps[j - 1].astype(jnp.bfloat16)
            ag_out[c, j - 1, 1] = scale.astype(jnp.bfloat16)
        for j in range(1, chips):
            at = c * (chips - 1) + j - 1
            third[c].append(
                send(
                    ag_out.at[c, j - 1],
                    ag_in.at[c, j - 1],
                    s3.at[at],
                    r3.at[at],
                    ahead(chips - j) * 2 + core,
                )
            )

    def collect(c):
        for copy in third[c]:
            copy.wait_recv()
        for j in range(1, chips):
            gap = ag_in[c, j - 1, 0].astype(jnp.float32)
            mean = total_of(part, c, j - 1) * (1.0 / share) + gap
            keep(span(c, core, ahead(j)), mean, ag_in[c, j - 1, 1])
        block = stats.at[:, halves(c, core)]
        fourth[c] = send(block, block, s4.at[c], r4.at[c], sibling)

    def transform(c):
        fourth[c].wait_recv()
        at = slice(c * height, (c + 1) * height)

        def body(i, carry):
            sides = [[], []]
            for u in range(TOGETHER):
                ch = i * TOGETHER + u
                value = (x_ref[ch, at, :] - stats[0, at, :]) - stats[1, at, :]
                normed = value * stats[2, at, :]
                left, right = normed[:, :half_c], normed[:, half_c:]
                sides[0].append(left + right)
                sides[1].append(left - right)
            for side in range(2):
                along = jnp.dot(
                    jnp.concatenate(sides[side], axis=0),
                    fwd_ref[side],
                    preferred_element_type=jnp.float32,
                )
                along_ref[
                    pl.ds(i * TOGETHER, TOGETHER), at, side * half_c : (side + 1) * half_c
                ] = along.reshape(TOGETHER, height, half_c).astype(jnp.bfloat16)
            return carry

        lax.fori_loop(0, local_ch // TOGETHER, body, 0)

    stages = (add_local, add_chip, finish, collect, transform)
    for tick in range(CHUNKS + sum(STARTS)):
        for stage_of, start in zip(stages, STARTS):
            if 0 <= tick - start < CHUNKS:
                stage_of(tick - start)
    for c in range(CHUNKS):
        for copy in [first[c], fourth[c]] + second[c] + third[c]:
            copy.wait_send()


def token_rows(fields, fwd, n):
    local_ch, rows, cols = fields.shape
    chips = n // 2
    height = rows // CHUNKS
    half, piece = height // 2, height // n
    counts = (CHUNKS, CHUNKS * (chips - 1), CHUNKS * (chips - 1), CHUNKS)
    f32, bf16 = jnp.float32, jnp.bfloat16
    return pl.pallas_call(
        functools.partial(token_kernel, n),
        out_shape=[pltpu.VMEM(fields.shape, bf16)] * 2,
        in_specs=[
            pl.BlockSpec(memory_space=pl.ANY),
            pl.BlockSpec(memory_space=pltpu.VMEM),
        ],
        out_specs=[pl.BlockSpec(memory_space=pltpu.VMEM)] * 2,
        scratch_shapes=[
            pltpu.VMEM((2, rows, cols), f32),
            pltpu.VMEM((3, rows, cols), bf16),
            pltpu.VMEM((CHUNKS, 2, half, cols), f32),
            pltpu.VMEM((CHUNKS, chips, 3, piece, cols), bf16),
            pltpu.VMEM((CHUNKS, chips - 1, 3, piece, cols), bf16),
            pltpu.VMEM((CHUNKS, chips - 1, 2, piece, cols), bf16),
            pltpu.VMEM((CHUNKS, chips - 1, 2, piece, cols), bf16),
            pltpu.SemaphoreType.DMA((CHUNKS,)),
        ]
        + [pltpu.SemaphoreType.DMA((c,)) for c in counts for _ in range(2)],
        compiler_params=pltpu.CompilerParams(
            collective_id=0, has_side_effects=True, vmem_limit_bytes=28 * 1024 * 1024
        ),
        name="tokens",
    )(fields, fwd)


def mix_pair(a_ref, b_ref, w_ref, b1_ref, odd, start, groups, edge):
    width, rows, cols = b_ref.shape
    half_r, half_c = rows // 2, cols // 2
    sums, gaps = [], []
    for g in range(2):
        mixed = []
        for side in range(2):
            values = a_ref[(2 * odd + side) * groups + start + g]
            hid = jnp.dot(w_ref[side], values, preferred_element_type=jnp.float32)
            hid = (hid + b1_ref[...]).astype(jnp.bfloat16)
            hid = jnp.maximum(hid, jnp.zeros_like(hid))
            out = jnp.dot(w_ref[2 + side], hid, preferred_element_type=jnp.float32)
            mixed.append((out - jnp.clip(out, -0.01, 0.01)).reshape(width, SUB, half_c))
        total, gap = mixed[0] + mixed[1], mixed[0] - mixed[1]
        if edge is not None and g == 0:
            line = lax.broadcasted_iota(jnp.int32, total.shape, 1)
            moved = pltpu.roll(mixed[1], SETS, 1)
            re_edge, im_edge = (line == 0) & edge, (line == SETS) & edge
            total = jnp.where(re_edge, mixed[0], jnp.where(im_edge, moved, total))
            gap = jnp.where(re_edge, -moved, jnp.where(im_edge, mixed[0], gap))
        sums.append(total)
        gaps.append(gap)
    spot = pl.ds(pl.multiple_of(odd * half_r + start * SUB, 2 * SUB), 2 * SUB)
    for i, parts in enumerate((sums, gaps)):
        b_ref[:, spot, i * half_c : (i + 1) * half_c] = jnp.concatenate(parts, axis=1).astype(
            jnp.bfloat16
        )


def return_rows(x_ref, b_ref, channel, back_ref, inv_ref, out_ref):
    local_ch, rows, cols = x_ref.shape
    half_r, half_c = rows // 2, cols // 2
    quarter = half_c // 2
    parts = []
    for p in range(2):
        even, odd = (
            jnp.dot(
                back_ref[2 * i + p],
                b_ref[channel, i * half_r : (i + 1) * half_r, p * half_c : (p + 1) * half_c],
                preferred_element_type=jnp.float32,
            )
            for i in range(2)
        )
        parts.append(jnp.concatenate([even + odd, even - odd], axis=0).astype(jnp.bfloat16))
    even, odd = (
        jnp.dot(
            jnp.concatenate([t[:, i * quarter : (i + 1) * quarter] for t in parts], axis=1),
            inv_ref[i],
            preferred_element_type=jnp.float32,
        )
        for i in range(2)
    )
    for i, filtered in enumerate((even + odd, even - odd)):
        span = slice(i * half_c, (i + 1) * half_c)
        for j in range(2):
            line = slice(j * half_r, (j + 1) * half_r)
            out_ref[(2 * j + i) * local_ch + channel] = (
                x_ref[channel, line, span].astype(jnp.float32) + filtered[line]
            ).astype(jnp.bfloat16)


def main_kernel(
    plan,
    x_ref,
    along_in,
    gain_ref,
    shift_ref,
    first_ref,
    second_ref,
    bias_ref,
    turn_hbm,
    back_hbm,
    inv_hbm,
    out_hbm,
    b_ref,
    a_ref,
    turn_ref,
    back_ref,
    inv_ref,
    w_ref,
    b1_ref,
    store_sem,
    table_sem,
):
    count, minis = plan
    local_ch, rows, cols = x_ref.shape
    steps = local_ch // count
    half_r, half_c = rows // 2, cols // 2
    groups = half_r // SUB
    index = lax.axis_index("grid")
    tables = [
        pltpu.make_async_copy(source, target, table_sem.at[i])
        for i, (source, target) in enumerate(
            ((turn_hbm, turn_ref), (back_hbm, back_ref), (inv_hbm, inv_ref))
        )
    ]

    def result(i):
        at = pl.ds(i * count, count)
        return [
            pltpu.make_async_copy(
                a_ref.at[pl.ds((2 * j + k) * local_ch + i * count, count)],
                out_hbm.at[
                    at, j * half_r : (j + 1) * half_r, k * half_c : (k + 1) * half_c
                ],
                store_sem.at[i * 4 + 2 * j + k],
            )
            for j in range(2)
            for k in range(2)
        ]

    for table in tables:
        table.start()
    prepare(index, gain_ref, first_ref, second_ref, bias_ref, w_ref, b1_ref)
    tables[0].wait()
    lift_scale = float(cols * rows) * float(fwd_first(cols)) * float(fwd_first(rows))

    def lift(channel):
        return shift_ref[channel] / gain_ref[channel] * lift_scale

    def forward(i, carry):
        for n in range(0, count, 2):
            here = i * count + n
            pair = [
                turn_rows(b_ref, here + u, turn_ref, lift(index * local_ch + here + u))
                for u in range(2)
            ]
            spot = pl.ds(pl.multiple_of(here * SUB, 2 * SUB), 2 * SUB)
            for kind in range(4):
                both = [p[kind].reshape(groups, SUB, -1) for p in pair]
                a_ref[kind * groups : (kind + 1) * groups, spot, :] = jnp.concatenate(
                    both, axis=1
                ).astype(jnp.bfloat16)
        return carry

    lax.fori_loop(0, steps, forward, 0)

    def mix(i, carry):
        for u in range(minis):
            mini = i * minis + u
            odd, start = lax.div(mini, groups // 2), 2 * lax.rem(mini, groups // 2)
            mix_pair(
                a_ref, b_ref, w_ref, b1_ref, odd, start, groups, i == 0 if u == 0 else None
            )
        return carry

    lax.fori_loop(0, groups // minis, mix, 0)
    for table in tables[1:]:
        table.wait()

    def backward(i, carry):
        for n in range(count):
            return_rows(x_ref, b_ref, i * count + n, back_ref, inv_ref, a_ref)
        for copy in result(i):
            copy.start()
        return carry

    lax.fori_loop(0, steps, backward, 0)
    for i in range(steps):
        for copy in result(i):
            copy.wait()


def fwd_first(size):
    return np.asarray(np.float32(1.0 / math.sqrt(size))).astype(jnp.bfloat16).astype(np.float32)


def per_device_local(fields, norm_gain, norm_shift, first_weight, second_weight, first_bias):
    local_ch, rows, cols = fields.shape
    half_r, half_c = rows // 2, cols // 2
    fwd, *tables = (jnp.asarray(t) for t in split_tables(rows, cols))
    near = pltpu.VMEM
    kept = [
        pltpu.with_memory_space_constraint(t, near)
        for t in token_rows(fields, fwd, lax.axis_size("grid"))
    ]
    size = first_weight.shape[2] * SUB
    count, minis = 4, 16
    steps = local_ch // count
    smem = pl.BlockSpec(memory_space=pltpu.SMEM)
    far = pl.BlockSpec(memory_space=pl.ANY)
    held = pl.BlockSpec(memory_space=near)
    result, _ = pl.pallas_call(
        functools.partial(main_kernel, (count, minis)),
        out_shape=[jax.ShapeDtypeStruct(fields.shape, jnp.bfloat16)]
        + [near(fields.shape, jnp.bfloat16)],
        in_specs=[held, held, smem, smem, held, held, held, far, far, far],
        out_specs=[far, held],
        input_output_aliases={1: 1},
        scratch_shapes=[
            pltpu.VMEM((4 * half_r // SUB, size, half_c), jnp.bfloat16),
        ]
        + [pltpu.VMEM(t.shape, jnp.bfloat16) for t in tables]
        + [
            pltpu.VMEM((4, size, size), jnp.bfloat16),
            pltpu.VMEM((size, half_c), jnp.float32),
        ]
        + [pltpu.SemaphoreType.DMA((c,)) for c in (4 * steps, 3)],
        compiler_params=pltpu.CompilerParams(vmem_limit_bytes=28 * 1024 * 1024),
        cost_estimate=pl.CostEstimate(
            flops=6 * fields.size * rows, bytes_accessed=6 * fields.size, transcendentals=0
        ),
        name="main",
    )(*kept, norm_gain, norm_shift, first_weight, second_weight, first_bias, *tables)
    return result


def per_device_any(fields, norm_gain, norm_shift, first_weight, second_weight, first_bias):
    local_ch, rows, cols = fields.shape
    groups = lax.axis_size("grid")
    one_block = local_ch == first_weight.shape[2] and local_ch % TOGETHER == 0
    tiled = rows % 256 == 0 and cols % 512 == 0 and local_ch * rows * cols <= 8 * 1024 * 1024
    tiled = tiled and SUB * local_ch == rows // 2 and groups % 2 == 0 and groups >= 4 and rows % (64 * groups) == 0
    chosen = per_device_local if one_block and tiled else per_device
    return chosen(fields, norm_gain, norm_shift, first_weight, second_weight, first_bias)


def solution(mesh):
    return jax.shard_map(
        per_device_any,
        mesh=mesh,
        in_specs=(P(("batch", "grid"), None, None), P(), P(), P(), P(), P()),
        out_specs=P(("batch", "grid"), None, None),
        check_vma=False,
    )
```

```python
import functools
import math

import jax
import jax.numpy as jnp
import numpy as np
from jax import lax
from jax.experimental import pallas as pl
from jax.experimental.pallas import tpu as pltpu
from jax.sharding import PartitionSpec as P


def tables(rows, cols):
    half = cols // 2
    col_index = jnp.arange(cols, dtype=jnp.int32)
    mode_index = jnp.arange(half, dtype=jnp.int32)
    angle_w = (col_index[:, None] * mode_index[None, :] % cols).astype(jnp.float32) * (
        2.0 * math.pi / cols
    )
    scale_w = 1.0 / math.sqrt(cols)
    fwd_w = jnp.concatenate(
        [jnp.cos(angle_w) * scale_w, -jnp.sin(angle_w) * scale_w], axis=1
    ).astype(jnp.bfloat16)
    weight_k = jnp.where(mode_index == 0, 1.0, 2.0).astype(jnp.float32)
    inv_w = jnp.concatenate(
        [
            (jnp.cos(angle_w) * weight_k[None, :] * scale_w).T,
            (-jnp.sin(angle_w) * weight_k[None, :] * scale_w).T,
        ],
        axis=0,
    ).astype(jnp.bfloat16)
    row_index = jnp.arange(rows, dtype=jnp.int32)
    angle_h = (row_index[:, None] * row_index[None, :] % rows).astype(jnp.float32) * (
        2.0 * math.pi / rows
    )
    scale_h = 1.0 / math.sqrt(rows)
    cos_h = (jnp.cos(angle_h) * scale_h).astype(jnp.bfloat16)
    sin_h = (jnp.sin(angle_h) * scale_h).astype(jnp.bfloat16)
    return (fwd_w, inv_w, cos_h, sin_h)


def mult(form, left, right):
    return jnp.einsum(form, left, right, preferred_element_type=jnp.float32)


def shrink(values):
    return jnp.maximum(values - 0.01, 0.0) + jnp.minimum(values + 0.01, 0.0)


def mix_modes(real_part, imag_part, first_weight, second_weight, first_bias):
    blocks = first_weight.shape[1]
    width = first_weight.shape[2]
    shape = real_part.shape
    real_blk = real_part.reshape(blocks, width, -1)
    imag_blk = imag_part.reshape(blocks, width, -1)
    bias_blk = first_bias.reshape(2, blocks, width, 1)
    hid_re = jax.nn.relu(
        mult("bio,bim->bom", first_weight[0], real_blk)
        - mult("bio,bim->bom", first_weight[1], imag_blk)
        + bias_blk[0]
    ).astype(jnp.bfloat16)
    hid_im = jax.nn.relu(
        mult("bio,bim->bom", first_weight[0], imag_blk)
        + mult("bio,bim->bom", first_weight[1], real_blk)
        + bias_blk[1]
    ).astype(jnp.bfloat16)
    out_re = mult("bio,bim->bom", second_weight[0], hid_re) - mult(
        "bio,bim->bom", second_weight[1], hid_im
    )
    out_im = mult("bio,bim->bom", second_weight[0], hid_im) + mult(
        "bio,bim->bom", second_weight[1], hid_re
    )
    return (
        shrink(out_re).astype(jnp.bfloat16).reshape(shape),
        shrink(out_im).astype(jnp.bfloat16).reshape(shape),
    )


def per_device(fields, norm_gain, norm_shift, first_weight, second_weight, first_bias):
    local_ch, rows, cols = fields.shape
    half = cols // 2
    groups = lax.axis_size("grid")
    channels = local_ch * groups
    fwd_w, inv_w, cos_h, sin_h = tables(rows, cols)
    values = fields.astype(jnp.float32)
    start = lax.axis_index("grid") * local_ch
    gain_own = lax.dynamic_slice_in_dim(norm_gain, start, local_ch)
    shift_own = lax.dynamic_slice_in_dim(norm_shift, start, local_ch)
    total_sum, total_sq = lax.psum(
        (jnp.sum(values, axis=0), jnp.sum(values * values, axis=0)), "grid"
    )
    mean = total_sum / channels
    var = total_sq / channels - mean * mean
    normed = (
        (values - mean) * lax.rsqrt(var + 1e-05) * gain_own[:, None, None]
        + shift_own[:, None, None]
    ).astype(jnp.bfloat16)
    along_w = (
        mult("chw,wk->chk", normed, fwd_w).astype(jnp.bfloat16).reshape(local_ch, rows, 2, half)
    )
    first_p = mult("kh,chpq->ckpq", cos_h, along_w)
    first_q = mult("kh,chpq->ckpq", sin_h, along_w)
    modes = jnp.stack(
        [
            (first_p[:, :, 0] + first_q[:, :, 1]).astype(jnp.bfloat16),
            (first_p[:, :, 1] - first_q[:, :, 0]).astype(jnp.bfloat16),
        ],
        axis=2,
    )
    spread = lax.all_to_all(modes, "grid", split_axis=1, concat_axis=0, tiled=True)
    shr_re, shr_im = mix_modes(
        spread[:, :, 0], spread[:, :, 1], first_weight, second_weight, first_bias
    )
    gathered = lax.all_to_all(
        jnp.stack([shr_re, shr_im], axis=2), "grid", split_axis=0, concat_axis=1, tiled=True
    )
    back_p = mult("kh,ckpq->chpq", cos_h, gathered)
    back_q = mult("kh,ckpq->chpq", sin_h, gathered)
    back_re = (back_p[:, :, 0] - back_q[:, :, 1]).astype(jnp.bfloat16)
    back_im = (back_p[:, :, 1] + back_q[:, :, 0]).astype(jnp.bfloat16)
    backed = jnp.concatenate([back_re, back_im], axis=2)
    filtered = mult("chk,kw->chw", backed, inv_w)
    return (values + filtered).astype(jnp.bfloat16)

SUB = 8


LANE = 128
SETS = 4


def wave(f, left, right, period):
    return f(
        (left[:, None] * right[None, :] % period).astype(np.float32)
        * np.float32(2.0 * math.pi / period)
    ) * np.float32(1.0 / math.sqrt(period))


def split_tables(rows, cols):
    half_r, half_c = rows // 2, cols // 2
    col, mode = np.arange(half_c), 2 * np.arange(half_c // 2)
    fwd, inv = [], []
    for odd in range(2):
        cos_w, sin_w = (wave(f, col, mode + odd, cols) for f in (np.cos, np.sin))
        fwd.append(np.concatenate([cos_w, -sin_w], axis=1))
        weight = np.where(mode + odd == 0, 1.0, 2.0).astype(np.float32)[:, None]
        inv.append(np.concatenate([cos_w.T * weight, -sin_w.T * weight], axis=0))
    row, pair = np.arange(half_r), 2 * np.arange(rows // 4)
    turn = []
    for odd in range(2):
        cos_h, sin_h = (wave(f, pair + odd, row, rows) for f in (np.cos, np.sin))
        on_re, on_im = [cos_h, -sin_h], [sin_h, cos_h]
        if odd == 0:
            middle = wave(np.cos, np.array([half_r]), row, rows)[0]
            on_re[1][0] = middle
            on_im[0] = on_im[0].copy()
            on_im[0][0] = middle
        for parts in (on_re, on_im):
            blocks = [p.reshape(-1, SETS, half_r) for p in parts]
            turn.append(np.concatenate(blocks, axis=1).reshape(half_r, half_r))
    turn = np.stack(turn)
    tables = (np.stack(fwd), turn, turn.transpose(0, 2, 1), np.stack(inv))
    return tuple(np.ascontiguousarray(t).astype(jnp.bfloat16) for t in tables)


def turn_rows(along_ref, n, turn_ref, lift):
    rows, cols = along_ref.shape[1:]
    half_r, half_c = rows // 2, cols // 2
    quarter = half_c // 2
    along = [
        jnp.concatenate(
            [
                along_ref[n, :, i * half_c + p * quarter : i * half_c + (p + 1) * quarter]
                for i in range(2)
            ],
            axis=1,
        )
        for p in range(2)
    ]
    out = []
    for odd in range(2):
        turned = []
        for p in range(2):
            top, low = along[p][:half_r], along[p][half_r:]
            part = top - low if odd else top + low
            turned.append(
                jnp.dot(turn_ref[2 * odd + p], part, preferred_element_type=jnp.float32)
            )
        plus, minus = turned[0] + turned[1], turned[0] - turned[1]
        if odd == 0:
            first, second = turned[0][:SUB], turned[1][:SUB]
            line = lax.broadcasted_iota(jnp.int32, first.shape, 0)
            lane = lax.broadcasted_iota(jnp.int32, first.shape, 1)
            head = jnp.where(line == 0, first, jnp.where(line == SETS, second, plus[:SUB]))
            head = head + jnp.where((line == 0) & (lane == 0), lift, 0.0)
            tail = jnp.where(
                line == 0,
                pltpu.roll(first, SETS, 0),
                jnp.where(line == SETS, -pltpu.roll(second, SETS, 0), minus[:SUB]),
            )
            plus = jnp.concatenate([head, plus[SUB:]], axis=0)
            minus = jnp.concatenate([tail, minus[SUB:]], axis=0)
        out += [plus, minus]
    return out


def wide_weight(real, imag, flip_in, flip_out):
    size = real.shape[0]
    rows = lax.broadcasted_iota(jnp.int32, (size * SUB, size), 0)
    cols = lax.broadcasted_iota(jnp.int32, (size * SUB, size), 1)
    repeat = jnp.where((rows >= cols * SUB) & (rows < cols * SUB + SUB), 1.0, 0.0).astype(
        jnp.bfloat16
    )
    last = (((1,), (1,)), ((), ()))
    full = []
    for weight in (real, imag):
        tall = lax.dot_general(repeat, weight, last, preferred_element_type=jnp.float32)
        full.append(
            lax.dot_general(
                tall.astype(jnp.bfloat16), repeat, last, preferred_element_type=jnp.float32
            )
        )
    left = lax.broadcasted_iota(jnp.int32, full[0].shape, 0)
    right = lax.broadcasted_iota(jnp.int32, full[0].shape, 1)
    same = ((left ^ right) & (SETS - 1)) == 0
    im_out, im_in = (left & SETS) != 0, (right & SETS) != 0
    value = jnp.where(
        im_out, jnp.where(im_in, full[0], full[1]), jnp.where(im_in, -full[1], full[0])
    )
    value = jnp.where(same, value, 0.0)
    flips = []
    for flip_i, flip_o in ((False, False), (flip_in, flip_out)):
        turned = jnp.where(im_in, -value, value) if flip_i else value
        flips.append(jnp.where(im_out, -turned, turned) if flip_o else turned)
    return [f.astype(jnp.bfloat16) for f in flips]


def prepare(block, gain_ref, first_ref, second_ref, bias_ref, w_ref, b1_ref):
    width = first_ref.shape[2]
    size = width * SUB
    row = lax.broadcasted_iota(jnp.int32, (width, width), 0)
    gain = jnp.zeros((width, width), jnp.float32)
    for i in range(width):
        gain = jnp.where(row == i, gain_ref[block * width + i], gain)
    for i, (source, flip) in enumerate(((first_ref, True), (second_ref, False))):
        parts = [source[p, block] for p in range(2)]
        if i == 0:
            parts = [(p.astype(jnp.float32) * gain).astype(jnp.bfloat16) for p in parts]
        pair = wide_weight(*parts, flip, not flip)
        for j in range(2):
            w_ref[2 * i + j] = pair[j]
    shape = (size, bias_ref.shape[1])
    line = lax.broadcasted_iota(jnp.int32, shape, 0)
    offset = line - (lax.broadcasted_iota(jnp.int32, shape, 1) - block * width) * SUB
    own = (offset >= 0) & (offset < SUB)
    picked = jnp.where((line & SETS) == 0, bias_ref[0:1, :], bias_ref[1:2, :])
    column = jnp.sum(jnp.where(own, picked, 0.0), axis=1, keepdims=True)
    b1_ref[...] = jnp.broadcast_to(column, b1_ref.shape)


CHUNKS = 8
STARTS = (0, 1, 4, 7, 9)
TOGETHER = 32


def token_kernel(
    n,
    x_hbm,
    fwd_ref,
    x_ref,
    along_ref,
    sums,
    stats,
    near,
    part,
    far,
    ag_out,
    ag_in,
    load_sem,
    s1,
    r1,
    s2,
    r2,
    s3,
    r3,
    s4,
    r4,
):
    me = lax.axis_index("grid")
    chips = n // 2
    core, chip = lax.rem(me, 2), lax.div(me, 2)
    sibling = chip * 2 + 1 - core
    local_ch, rows, cols = x_ref.shape
    half_c = cols // 2
    height = rows // CHUNKS
    half, piece = height // 2, cols // chips
    share = 2.0 * local_ch

    def ahead(j):
        return lax.rem(chip + j, chips)

    def halves(c, owner):
        return pl.ds(pl.multiple_of(c * height + owner * half, half), half)

    def lanes(k):
        return pl.ds(pl.multiple_of(k * piece, piece), piece)

    def total_of(ref, c, j):
        return ref[c, j, 0].astype(jnp.float32) + ref[c, j, 1].astype(jnp.float32)

    def keep(c, k, mean, scale):
        high = mean.astype(jnp.bfloat16)
        low = (mean - high.astype(jnp.float32)).astype(jnp.bfloat16)
        for i, plane in enumerate((high, low, scale)):
            stats[i, halves(c, core), lanes(k)] = plane

    def send(source, target, send_sem, recv_sem, device):
        copy = pltpu.make_async_remote_copy(
            src_ref=source,
            dst_ref=target,
            send_sem=send_sem,
            recv_sem=recv_sem,
            device_id={"grid": device},
            device_id_type=pl.DeviceIdType.MESH,
        )
        copy.start()
        return copy

    loads = [
        pltpu.make_async_copy(
            x_hbm.at[:, c * height : (c + 1) * height],
            x_ref.at[:, c * height : (c + 1) * height],
            load_sem.at[c],
        )
        for c in range(CHUNKS)
    ]
    for copy in loads:
        copy.start()
    barrier = pltpu.get_barrier_semaphore()
    for device in [sibling] + [ahead(j) * 2 + core for j in range(1, chips)]:
        pl.semaphore_signal(
            barrier, inc=1, device_id={"grid": device}, device_id_type=pl.DeviceIdType.MESH
        )

    first, second, third, fourth = {}, {}, {}, {}

    def add_local(c):
        loads[c].wait()
        lines = 2 * SUB

        def body(r, carry):
            at = pl.ds(pl.multiple_of(c * height + r * lines, lines), lines)
            total = jnp.zeros((lines, cols), jnp.float32)
            square = jnp.zeros((lines, cols), jnp.float32)
            for ch in range(local_ch):
                value = x_ref[ch, at, :].astype(jnp.float32)
                total = total + value
                square = square + value * value
            sums[0, at, :] = total
            sums[1, at, :] = square
            return carry

        lax.fori_loop(0, height // lines, body, 0)
        if c == 0:
            pl.semaphore_wait(barrier, chips)
        first[c] = send(
            sums.at[:, halves(c, 1 - core)], near.at[c], s1.at[c], r1.at[c], sibling
        )

    def add_chip(c):
        first[c].wait_recv()
        for j in range(1, chips + 1):
            at = lanes(ahead(j))
            total = sums[0, halves(c, core), at] + near[c, 0, :, at]
            square = sums[1, halves(c, core), at] + near[c, 1, :, at]
            high = total.astype(jnp.bfloat16)
            low = (total - high.astype(jnp.float32)).astype(jnp.bfloat16)
            spread = (square - total * total * (1.0 / share)).astype(jnp.bfloat16)
            for i, plane in enumerate((high, low, spread)):
                part[c, j - 1, i] = plane
        second[c] = []
        for j in range(1, chips):
            at = c * (chips - 1) + j - 1
            second[c].append(
                send(
                    part.at[c, j - 1],
                    far.at[c, j - 1],
                    s2.at[at],
                    r2.at[at],
                    ahead(j) * 2 + core,
                )
            )

    def finish(c):
        for copy in second[c]:
            copy.wait_recv()
        own = total_of(part, c, chips - 1)
        others = [total_of(far, c, j) for j in range(chips - 1)]
        total = own
        for other in others:
            total = total + other
        mean = total * (1.0 / (share * chips))
        spread = part[c, chips - 1, 2].astype(jnp.float32)
        for j in range(chips - 1):
            spread = spread + far[c, j, 2].astype(jnp.float32)
        gaps = [mean - other * (1.0 / share) for other in others]
        for gap in gaps + [mean - own * (1.0 / share)]:
            spread = spread + gap * gap * share
        scale = lax.rsqrt(spread * (1.0 / (share * chips)) + 1e-05)
        keep(c, chip, mean, scale.astype(jnp.bfloat16))
        third[c] = []
        for j in range(1, chips):
            ag_out[c, j - 1, 0] = gaps[j - 1].astype(jnp.bfloat16)
            ag_out[c, j - 1, 1] = scale.astype(jnp.bfloat16)
        for j in range(1, chips):
            at = c * (chips - 1) + j - 1
            third[c].append(
                send(
                    ag_out.at[c, j - 1],
                    ag_in.at[c, j - 1],
                    s3.at[at],
                    r3.at[at],
                    ahead(chips - j) * 2 + core,
                )
            )

    def collect(c):
        for copy in third[c]:
            copy.wait_recv()
        for j in range(1, chips):
            gap = ag_in[c, j - 1, 0].astype(jnp.float32)
            mean = total_of(part, c, j - 1) * (1.0 / share) + gap
            keep(c, ahead(j), mean, ag_in[c, j - 1, 1])
        block = stats.at[:, halves(c, core)]
        fourth[c] = send(block, block, s4.at[c], r4.at[c], sibling)

    def transform(c):
        fourth[c].wait_recv()
        at = slice(c * height, (c + 1) * height)

        def body(i, carry):
            sides = [[], []]
            for u in range(TOGETHER):
                ch = i * TOGETHER + u
                value = (x_ref[ch, at, :] - stats[0, at, :]) - stats[1, at, :]
                normed = value * stats[2, at, :]
                left, right = normed[:, :half_c], normed[:, half_c:]
                sides[0].append(left + right)
                sides[1].append(left - right)
            for side in range(2):
                along = jnp.dot(
                    jnp.concatenate(sides[side], axis=0),
                    fwd_ref[side],
                    preferred_element_type=jnp.float32,
                )
                along_ref[
                    pl.ds(i * TOGETHER, TOGETHER), at, side * half_c : (side + 1) * half_c
                ] = along.reshape(TOGETHER, height, half_c).astype(jnp.bfloat16)
            return carry

        lax.fori_loop(0, local_ch // TOGETHER, body, 0)

    stages = (add_local, add_chip, finish, collect, transform)
    for tick in range(CHUNKS + STARTS[-1]):
        for stage_of, start in zip(stages, STARTS):
            if 0 <= tick - start < CHUNKS:
                stage_of(tick - start)
    for c in range(CHUNKS):
        for copy in [first[c], fourth[c]] + second[c] + third[c]:
            copy.wait_send()


def token_rows(fields, fwd, n):
    local_ch, rows, cols = fields.shape
    chips = n // 2
    height = rows // CHUNKS
    half, piece = height // 2, cols // chips
    counts = (CHUNKS, CHUNKS * (chips - 1), CHUNKS * (chips - 1), CHUNKS)
    f32, bf16 = jnp.float32, jnp.bfloat16
    return pl.pallas_call(
        functools.partial(token_kernel, n),
        out_shape=[pltpu.VMEM(fields.shape, bf16)] * 2,
        in_specs=[
            pl.BlockSpec(memory_space=pl.ANY),
            pl.BlockSpec(memory_space=pltpu.VMEM),
        ],
        out_specs=[pl.BlockSpec(memory_space=pltpu.VMEM)] * 2,
        scratch_shapes=[
            pltpu.VMEM((2, rows, cols), f32),
            pltpu.VMEM((3, rows, cols), bf16),
            pltpu.VMEM((CHUNKS, 2, half, cols), f32),
            pltpu.VMEM((CHUNKS, chips, 3, half, piece), bf16),
            pltpu.VMEM((CHUNKS, chips - 1, 3, half, piece), bf16),
            pltpu.VMEM((CHUNKS, chips - 1, 2, half, piece), bf16),
            pltpu.VMEM((CHUNKS, chips - 1, 2, half, piece), bf16),
            pltpu.SemaphoreType.DMA((CHUNKS,)),
        ]
        + [pltpu.SemaphoreType.DMA((c,)) for c in counts for _ in range(2)],
        compiler_params=pltpu.CompilerParams(
            collective_id=0, has_side_effects=True, vmem_limit_bytes=28 * 1024 * 1024
        ),
        name="tokens",
    )(fields, fwd)


def mix_pair(a_ref, b_ref, w_ref, b1_ref, odd, start, groups, edge):
    width, rows, cols = b_ref.shape
    half_r, half_c = rows // 2, cols // 2
    sums, gaps = [], []
    for g in range(2):
        mixed = []
        for side in range(2):
            values = a_ref[(2 * odd + side) * groups + start + g]
            hid = jnp.dot(w_ref[side], values, preferred_element_type=jnp.float32)
            hid = (hid + b1_ref[...]).astype(jnp.bfloat16)
            hid = jnp.maximum(hid, jnp.zeros_like(hid))
            out = jnp.dot(w_ref[2 + side], hid, preferred_element_type=jnp.float32)
            mixed.append((out - jnp.clip(out, -0.01, 0.01)).reshape(width, SUB, half_c))
        total, gap = mixed[0] + mixed[1], mixed[0] - mixed[1]
        if edge is not None and g == 0:
            line = lax.broadcasted_iota(jnp.int32, total.shape, 1)
            moved = pltpu.roll(mixed[1], SETS, 1)
            re_edge, im_edge = (line == 0) & edge, (line == SETS) & edge
            total = jnp.where(re_edge, mixed[0], jnp.where(im_edge, moved, total))
            gap = jnp.where(re_edge, -moved, jnp.where(im_edge, mixed[0], gap))
        sums.append(total)
        gaps.append(gap)
    spot = pl.ds(pl.multiple_of(odd * half_r + start * SUB, 2 * SUB), 2 * SUB)
    for i, parts in enumerate((sums, gaps)):
        b_ref[:, spot, i * half_c : (i + 1) * half_c] = jnp.concatenate(parts, axis=1).astype(
            jnp.bfloat16
        )


def return_rows(x_ref, b_ref, channel, back_ref, inv_ref, out_ref):
    local_ch, rows, cols = x_ref.shape
    half_r, half_c = rows // 2, cols // 2
    quarter = half_c // 2
    parts = []
    for p in range(2):
        even, odd = (
            jnp.dot(
                back_ref[2 * i + p],
                b_ref[channel, i * half_r : (i + 1) * half_r, p * half_c : (p + 1) * half_c],
                preferred_element_type=jnp.float32,
            )
            for i in range(2)
        )
        parts.append(jnp.concatenate([even + odd, even - odd], axis=0).astype(jnp.bfloat16))
    even, odd = (
        jnp.dot(
            jnp.concatenate([t[:, i * quarter : (i + 1) * quarter] for t in parts], axis=1),
            inv_ref[i],
            preferred_element_type=jnp.float32,
        )
        for i in range(2)
    )
    for i, filtered in enumerate((even + odd, even - odd)):
        span = slice(i * half_c, (i + 1) * half_c)
        for j in range(2):
            line = slice(j * half_r, (j + 1) * half_r)
            out_ref[(2 * j + i) * local_ch + channel] = (
                x_ref[channel, line, span].astype(jnp.float32) + filtered[line]
            ).astype(jnp.bfloat16)


def main_kernel(
    plan,
    x_ref,
    along_in,
    gain_ref,
    shift_ref,
    first_ref,
    second_ref,
    bias_ref,
    turn_hbm,
    back_hbm,
    inv_hbm,
    out_hbm,
    b_ref,
    a_ref,
    turn_ref,
    back_ref,
    inv_ref,
    w_ref,
    b1_ref,
    store_sem,
    table_sem,
):
    count, minis, deep, sent = plan
    local_ch, rows, cols = x_ref.shape
    steps = local_ch // count
    half_r, half_c = rows // 2, cols // 2
    groups = half_r // SUB
    index = lax.axis_index("grid")
    tables = [
        pltpu.make_async_copy(source, target, table_sem.at[i])
        for i, (source, target) in enumerate(
            ((turn_hbm, turn_ref), (back_hbm, back_ref), (inv_hbm, inv_ref))
        )
    ]

    def result(i):
        at = pl.ds(i * sent, sent)
        return [
            pltpu.make_async_copy(
                a_ref.at[pl.ds((2 * j + k) * local_ch + i * sent, sent)],
                out_hbm.at[
                    at, j * half_r : (j + 1) * half_r, k * half_c : (k + 1) * half_c
                ],
                store_sem.at[i * 4 + 2 * j + k],
            )
            for j in range(2)
            for k in range(2)
        ]

    for table in tables:
        table.start()
    prepare(index, gain_ref, first_ref, second_ref, bias_ref, w_ref, b1_ref)
    tables[0].wait()
    lift_scale = float(cols * rows) * float(fwd_first(cols)) * float(fwd_first(rows))

    def lift(channel):
        return shift_ref[channel] / gain_ref[channel] * lift_scale

    def forward(i, carry):
        for n in range(0, count, 2):
            here = i * count + n
            pair = [
                turn_rows(b_ref, here + u, turn_ref, lift(index * local_ch + here + u))
                for u in range(2)
            ]
            spot = pl.ds(pl.multiple_of(here * SUB, 2 * SUB), 2 * SUB)
            for kind in range(4):
                both = [p[kind].reshape(groups, SUB, -1) for p in pair]
                a_ref[kind * groups : (kind + 1) * groups, spot, :] = jnp.concatenate(
                    both, axis=1
                ).astype(jnp.bfloat16)
        return carry

    lax.fori_loop(0, steps, forward, 0)

    def mix(i, carry):
        for u in range(minis):
            mini = i * minis + u
            odd, start = lax.div(mini, groups // 2), 2 * lax.rem(mini, groups // 2)
            mix_pair(
                a_ref, b_ref, w_ref, b1_ref, odd, start, groups, i == 0 if u == 0 else None
            )
        return carry

    lax.fori_loop(0, groups // minis, mix, 0)
    for table in tables[1:]:
        table.wait()

    def backward(i, carry):
        for n in range(0, deep, sent):
            for u in range(sent):
                return_rows(x_ref, b_ref, i * deep + n + u, back_ref, inv_ref, a_ref)
            for copy in result(i * (deep // sent) + n // sent):
                copy.start()
        return carry

    lax.fori_loop(0, local_ch // deep, backward, 0)
    for i in range(local_ch // sent):
        for copy in result(i):
            copy.wait()


def fwd_first(size):
    return np.asarray(np.float32(1.0 / math.sqrt(size))).astype(jnp.bfloat16).astype(np.float32)


def per_device_local(fields, norm_gain, norm_shift, first_weight, second_weight, first_bias):
    local_ch, rows, cols = fields.shape
    half_r, half_c = rows // 2, cols // 2
    fwd, *tables = (jnp.asarray(t) for t in split_tables(rows, cols))
    near = pltpu.VMEM
    kept = [
        pltpu.with_memory_space_constraint(t, near)
        for t in token_rows(fields, fwd, lax.axis_size("grid"))
    ]
    size = first_weight.shape[2] * SUB
    plan = (16, 16, 16, 4)
    parts = 4 * local_ch // plan[3]
    smem = pl.BlockSpec(memory_space=pltpu.SMEM)
    far = pl.BlockSpec(memory_space=pl.ANY)
    held = pl.BlockSpec(memory_space=near)
    result, _ = pl.pallas_call(
        functools.partial(main_kernel, plan),
        out_shape=[jax.ShapeDtypeStruct(fields.shape, jnp.bfloat16)]
        + [near(fields.shape, jnp.bfloat16)],
        in_specs=[held, held, smem, smem, held, held, held, far, far, far],
        out_specs=[far, held],
        input_output_aliases={1: 1},
        scratch_shapes=[
            pltpu.VMEM((4 * half_r // SUB, size, half_c), jnp.bfloat16),
        ]
        + [pltpu.VMEM(t.shape, jnp.bfloat16) for t in tables]
        + [
            pltpu.VMEM((4, size, size), jnp.bfloat16),
            pltpu.VMEM((size, half_c), jnp.float32),
        ]
        + [pltpu.SemaphoreType.DMA((c,)) for c in (parts, 3)],
        compiler_params=pltpu.CompilerParams(vmem_limit_bytes=28 * 1024 * 1024),
        cost_estimate=pl.CostEstimate(
            flops=6 * fields.size * rows, bytes_accessed=6 * fields.size, transcendentals=0
        ),
        name="main",
    )(*kept, norm_gain, norm_shift, first_weight, second_weight, first_bias, *tables)
    return result


def per_device_any(fields, norm_gain, norm_shift, first_weight, second_weight, first_bias):
    local_ch, rows, cols = fields.shape
    groups = lax.axis_size("grid")
    one_block = local_ch == first_weight.shape[2] and local_ch % TOGETHER == 0
    tiled = rows % 256 == 0 and cols % 512 == 0 and local_ch * rows * cols <= 8 * 1024 * 1024
    tiled = tiled and SUB * local_ch == rows // 2 and groups % 2 == 0 and groups >= 4 and cols % (LANE * groups // 2) == 0 and rows % (32 * CHUNKS) == 0
    chosen = per_device_local if one_block and tiled else per_device
    return chosen(fields, norm_gain, norm_shift, first_weight, second_weight, first_bias)


def solution(mesh):
    return jax.shard_map(
        per_device_any,
        mesh=mesh,
        in_specs=(P(("batch", "grid"), None, None), P(), P(), P(), P(), P()),
        out_specs=P(("batch", "grid"), None, None),
        check_vma=False,
    )
```
